768 devices in a mesh: face: 6 (over z_lo, core), tile: 128 (over x, y, z_hi).
Axes of the slice: x: 4, y: 8, z: 12 (z_hi: 4, z_lo: 3; z = z_hi * 3 + z_lo), core: 2. Of those that a mesh axis runs over, the one named last changes fastest.
Arguments:
- crm_state: bfloat16 [6, 72, 786432], P(None, None, ('face', 'tile')), may hold values from -4 to 4
- active_levels: int32 [24576], P(('face', 'tile')), may hold values from 18 to 72
- mix_x: float32 [24576], P(('face', 'tile')), may hold values from 0.05 to 0.2
- drift_speed: float32 [24576], P(('face', 'tile')), may hold values from -0.1 to 0.1
- cond_rate: float32 [24576], P(('face', 'tile')), may hold values from 0.2 to 0.8
- mix_z: float32 [72], replicated, may hold values from 0.02 to 0.2
- point_mass: float32 [98304], P(('face', 'tile')), may hold values from 0.3 to 3
- neighbor_slots: int32 [4, 6144], P(None, ('face', 'tile')), may hold values from 0 to 39, as said below
- edge_codes: int32 [4, 6144], P(None, ('face', 'tile')), may hold values from 0 to 7, as said below
Outputs:
- new_state: bfloat16 [6, 72, 786432], P(None, None, ('face', 'tile'))
- gll_tendency: float32 [6, 72, 98304], P(None, None, ('face', 'tile'))
The draws below stay inside these ranges and needn't reach their ends.
Inputs may be any that keep to these rules, and one draw needn't show every extreme that they name: `neighbor_slots`: v // 8 is 0 for this device, 1 for tile index - 1, 2 for tile index + 1, 3 for face index - 1, 4 for face index + 1 (indices wrapping), and v % 8 the element there. The relation is mutual: if e names b across one of its edges, b names e across one of its own. On every device exactly 4 elements name an element on tile index - 1, 4 on tile index + 1, 2 on face index - 1 and 2 on face index + 1, each exactly one such element. `edge_codes`: 2 k' + r: k' is the neighbour's own edge that is shared, and r is 1 when the two elements list that edge's cells and points in opposite senses. Codes agree from both sides of every edge.
All inputs are finite; a program needn't handle non-finite values.
Results may differ from the reference program's by a relative error of at most 0.001.
Values sent between devices are 32-bit elements; how exact they have to be, the bound alone decides.
A program may use at most 64 MiB of HBM per device.

```python
import math
import jax
import jax.numpy as jnp
import numpy as np
from jax import lax

FIELDS = 6
LEV = 72
CRMX = 32
NSUB = 2
BLK_R = 4
BLK_C = 2
E_DEV = 8
ELEMS = 6144
N_FACE = 6
N_TILE = 128


def element_graph(key):
    graph_key = jax.random.fold_in(key, 11)
    turn_key, order_key = jax.random.split(graph_key)
    devices = N_FACE * N_TILE
    rotation = jax.random.randint(turn_key, (ELEMS,), 0, 4).astype(jnp.int32)

    def shuffle(device_key):
        return jax.random.permutation(device_key, E_DEV).astype(jnp.int32)
    layout = jax.vmap(shuffle)(jax.random.split(order_key, devices))
    inverse = jnp.argsort(layout, axis=1).astype(jnp.int32)
    element = jnp.arange(ELEMS, dtype=jnp.int32)
    device = element // E_DEV
    grid_place = layout[device, element % E_DEV]
    grid_rows = N_FACE * BLK_R
    grid_cols = N_TILE * BLK_C
    row_index = device // N_TILE * BLK_R + grid_place // BLK_C
    col_index = device % N_TILE * BLK_C + grid_place % BLK_C
    edge_ids = jnp.arange(4, dtype=jnp.int32)[:, None]
    facing = (edge_ids + rotation[None, :]) % 4
    row_step = jnp.array([-1, 0, 1, 0], jnp.int32)[facing]
    col_step = jnp.array([0, 1, 0, -1], jnp.int32)[facing]
    other_row = (row_index[None, :] + row_step) % grid_rows
    other_col = (col_index[None, :] + col_step) % grid_cols
    other_device = other_row // BLK_R * N_TILE + other_col // BLK_C
    other_place = other_row % BLK_R * BLK_C + other_col % BLK_C
    other_slot = inverse[other_device, other_place]
    other_element = other_device * E_DEV + other_slot
    source = jnp.where(other_device == device[None, :], 0, jnp.where(facing == 3, 1, jnp.where(facing == 1, 2, jnp.where(facing == 0, 3, 4))))
    slot_values = source * E_DEV + other_slot
    back_edge = (facing + 2 - rotation[other_element]) % 4
    sign_table = jnp.array([[1, 1, -1, -1], [1, -1, -1, 1]], jnp.int32)
    own_sign = sign_table[edge_ids % 2, rotation[None, :]]
    other_sign = sign_table[back_edge % 2, rotation[other_element]]
    code_values = 2 * back_edge + (own_sign != other_sign).astype(jnp.int32)
    return (slot_values.astype(jnp.int32), code_values.astype(jnp.int32))


def draw_neighbor_slots(key, part):
    return element_graph(key)[0]


def draw_edge_codes(key, part):
    return element_graph(key)[1]


def place_ends(entries, own_key, least, largest):
    longest = entries.shape.index(max(entries.shape))
    spots = []
    for shift in (0, 1):
        where = [jax.random.randint(jax.random.fold_in(own_key, axis), (), 0, length) for axis, length in enumerate(entries.shape)]
        where[longest] = (where[longest] + shift) % entries.shape[longest]
        spots.append(tuple(where))
    return entries.at[spots[0]].set(least).at[spots[1]].set(largest)


def block_scale(own_key, shape, cuts, low, high):
    gain, own = 1.0, jax.random.fold_in(own_key, 6)
    for dim, shards_of in cuts:
        draws = jnp.exp(jax.random.uniform(jax.random.fold_in(own, dim), (shards_of,), jnp.float32, low / len(cuts), high / len(cuts)))
        gain = gain * jnp.repeat(draws, shape[dim] // shards_of).reshape([-1 if axis == dim else 1 for axis in range(len(shape))])
    return gain


def normal_values(own_key, shape, deviation, most, shards=(), kind=jnp.bfloat16):
    entries = deviation * jax.random.normal(own_key, shape, jnp.float32)
    if shards:
        entries = entries * block_scale(own_key, shape, shards, -0.22, 0.18)
    return jnp.clip(entries, -most, most).astype(kind)


def setup_inputs(seed: int = 0) -> dict:
    key_list = jax.random.split(jax.random.key(seed), 10)
    crm_state = normal_values(key_list[0], (FIELDS, LEV, 4 * ELEMS * CRMX), 1.0, 4.0, ((2, 768),))
    active_levels = place_ends(jax.random.randint(key_list[1], (4 * ELEMS,), LEV // 4, LEV + 1), jax.random.fold_in(key_list[1], 1), LEV // 4, LEV).astype(jnp.int32)
    mix_x = jnp.clip(jnp.exp(math.log(0.2) - 1.3862944 * jax.random.uniform(key_list[2], (4 * ELEMS,), jnp.float32) ** block_scale(key_list[2], (4 * ELEMS,), ((0, 768),), -0.2, 0.2)), 0.05, 0.2)
    drift_speed = jnp.clip(jax.random.uniform(key_list[3], (4 * ELEMS,), jnp.float32, -0.1, 0.1) * block_scale(key_list[3], (4 * ELEMS,), ((0, 768),), -0.4, 0.0), -0.1, 0.1)
    cond_rate = jnp.clip(jnp.exp(math.log(0.8) - 1.3862944 * jax.random.uniform(key_list[4], (4 * ELEMS,), jnp.float32) ** block_scale(key_list[4], (4 * ELEMS,), ((0, 768),), -0.2, 0.2)), 0.2, 0.8)
    mix_z = jnp.clip(jnp.exp(jax.random.uniform(key_list[5], (LEV,), jnp.float32, math.log(0.02), math.log(0.2))), 0.02, 0.2)
    point_mass = jnp.clip(jnp.exp(math.log(3.0) - 2.3025851 * jax.random.uniform(key_list[6], (16 * ELEMS,), jnp.float32) ** block_scale(key_list[6], (16 * ELEMS,), ((0, 768),), -0.2, 0.2)), 0.3, 3.0)
    neighbor_slots = draw_neighbor_slots(jax.random.fold_in(key_list[9], 71), 0)
    edge_codes = draw_edge_codes(jax.random.fold_in(key_list[9], 71), 0)
    return dict(crm_state=crm_state, active_levels=active_levels, mix_x=mix_x, drift_speed=drift_speed, cond_rate=cond_rate, mix_z=mix_z, point_mass=point_mass, neighbor_slots=neighbor_slots, edge_codes=edge_codes)


per_time = 10.0
CELL_EDGE = [[0, 1], [1, 3], [2, 3], [0, 2]]
GLL_EDGE = [[0, 1, 2, 3], [3, 7, 11, 15], [12, 13, 14, 15], [0, 4, 8, 12]]

def oriented(edge_lists):
    row_list = []
    for edge_code in range(8):
        edge_side = list(edge_lists[edge_code // 2])
        if edge_code % 2 == 1:
            edge_side = edge_side[::-1]
        row_list.append(edge_side)
    return np.array(row_list, np.int32)

def lagrange(q, z):
    centres = [-1.5, -0.5, 0.5, 1.5]
    product = 1.0
    for r in range(4):
        if r != q:
            product = product * (z - centres[r]) / (centres[q] - centres[r])
    return product

def linear_weight(j, z):
    return 0.5 - z if j == 0 else 0.5 + z

def remap_matrix():
    gll_nodes = [-1.0, -1.0 / math.sqrt(5.0), 1.0 / math.sqrt(5.0), 1.0]
    matrix = [[0.0 for column in range(12)] for row in range(16)]
    for b in range(4):
        for a in range(4):
            p = 4 * b + a
            x = gll_nodes[a]
            y = gll_nodes[b]
            for j in range(2):
                for i in range(2):
                    matrix[p][2 * j + i] += 0.5 * linear_weight(j, y) * lagrange(1 + i, x) + 0.5 * linear_weight(i, x) * lagrange(1 + j, y)
            for m in range(2):
                matrix[p][4 + 6 + m] += 0.5 * linear_weight(m, y) * lagrange(0, x)
                matrix[p][4 + 2 + m] += 0.5 * linear_weight(m, y) * lagrange(3, x)
                matrix[p][4 + 0 + m] += 0.5 * linear_weight(m, x) * lagrange(0, y)
                matrix[p][4 + 4 + m] += 0.5 * linear_weight(m, x) * lagrange(3, y)
    return np.array(matrix, np.float32)

def microphysics(prognostic_bundle, alive_indicator, cond_speed):
    thermal_profile = prognostic_bundle[0]
    gaseous_moisture = prognostic_bundle[1]
    cloud_droplets = prognostic_bundle[2]
    icy_hydrometeor = prognostic_bundle[3]
    humidity_ceiling = 0.5 * jnp.exp(0.3 * thermal_profile)
    droplet_growth_increment = jnp.where(alive_indicator, jnp.maximum(cond_speed * (gaseous_moisture - humidity_ceiling), -cloud_droplets), 0.0)
    gaseous_moisture = gaseous_moisture - droplet_growth_increment
    cloud_droplets = cloud_droplets + droplet_growth_increment
    thermal_profile = thermal_profile + 0.5 * droplet_growth_increment
    glaciation_increment = jnp.where(alive_indicator, 0.3 * cloud_droplets * jax.nn.sigmoid(-2.0 * thermal_profile), 0.0)
    cloud_droplets = cloud_droplets - glaciation_increment
    icy_hydrometeor = icy_hydrometeor + glaciation_increment
    thermal_profile = thermal_profile + 0.1 * glaciation_increment
    return jnp.stack([thermal_profile, gaseous_moisture, cloud_droplets, icy_hydrometeor, prognostic_bundle[4], prognostic_bundle[5]])

def crm_advance(prognostic_bundle, active, mix_x, drift_speed, cond_rate, mix_z):
    initial = prognostic_bundle.astype(jnp.float32)
    levels = initial.shape[1]
    alive_indicator = jnp.arange(levels, dtype=jnp.int32)[:, None, None] < active[None, :, None]
    coupling = jnp.where(jnp.arange(levels, dtype=jnp.int32) < levels - 1, mix_z, 0.0)[:, None, None]
    mix_horiz = mix_x[:, None]
    shift_rate = drift_speed[:, None]
    cond_speed = cond_rate[:, None]
    current = initial
    for substep in range(NSUB):
        east_side = jnp.roll(current, -1, axis=3)
        west_side = jnp.roll(current, 1, axis=3)
        current = current + mix_horiz * (east_side - 2.0 * current + west_side) + 0.5 * shift_rate * (west_side - east_side)
        level_above = jnp.concatenate([current[:, 1:], current[:, -1:]], axis=1)
        flux_up = coupling * (level_above - current)
        flux_below = jnp.concatenate([jnp.zeros_like(flux_up[:, :1]), flux_up[:, :-1]], axis=1)
        current = current + flux_up - flux_below
        current = microphysics(current, alive_indicator, cond_speed)
    return (current, lax.optimization_barrier(jnp.mean(current - initial, axis=3)) * per_time)

def reference(crm_state, active_levels, mix_x, drift_speed, cond_rate, mix_z, point_mass, neighbor_slots, edge_codes):
    columns = 4 * E_DEV
    blocks = ELEMS // E_DEV

    def advance_block(block_index):
        begin = block_index * columns
        piece = lax.dynamic_slice_in_dim(crm_state, begin * CRMX, columns * CRMX, 2).reshape(FIELDS, LEV, columns, CRMX)
        current, tendency = crm_advance(piece, lax.dynamic_slice_in_dim(active_levels, begin, columns, 0), lax.dynamic_slice_in_dim(mix_x, begin, columns, 0), lax.dynamic_slice_in_dim(drift_speed, begin, columns, 0), lax.dynamic_slice_in_dim(cond_rate, begin, columns, 0), mix_z)
        return (current.astype(jnp.bfloat16).reshape(FIELDS, LEV, columns * CRMX), tendency)
    states, tendencies = lax.map(advance_block, jnp.arange(blocks, dtype=jnp.int32))
    new_state = jnp.transpose(states, (1, 2, 0, 3)).reshape(FIELDS, LEV, 4 * ELEMS * CRMX)
    tendency = jnp.transpose(tendencies, (1, 2, 0, 3)).reshape(FIELDS, LEV, 4 * ELEMS)
    element = jnp.arange(ELEMS, dtype=jnp.int32)
    device = element // E_DEV
    face_index = device // N_TILE
    tile_index = device % N_TILE
    source = neighbor_slots // E_DEV
    position = neighbor_slots % E_DEV
    face_other = jnp.where(source == 3, (face_index - 1) % N_FACE, jnp.where(source == 4, (face_index + 1) % N_FACE, face_index))
    tile_other = jnp.where(source == 1, (tile_index - 1) % N_TILE, jnp.where(source == 2, (tile_index + 1) % N_TILE, tile_index))
    partner = ((face_other * N_TILE + tile_other) * E_DEV + position).astype(jnp.int32)
    cell_table = jnp.asarray(oriented(CELL_EDGE))
    cell_pick = jnp.take(cell_table, edge_codes, axis=0)
    gather_index = (partner[:, :, None] * 4 + cell_pick).transpose(1, 0, 2).reshape(-1).astype(jnp.int32)
    across = jnp.take(tendency, gather_index, axis=2).reshape(FIELDS, LEV, ELEMS, 8)
    stacked = jnp.concatenate([tendency.reshape(FIELDS, LEV, ELEMS, 4), across], axis=3)
    matrix = jnp.asarray(remap_matrix(), jnp.float32)
    gll = jnp.einsum('flec,pc->flep', stacked, matrix, precision=lax.Precision.HIGHEST)
    masses = point_mass.reshape(ELEMS, 16)
    weighted = gll * masses
    numerator = weighted
    denominator = masses
    flat_weighted = weighted.reshape(FIELDS, LEV, ELEMS * 16)
    flat_mass = point_mass
    point_table = jnp.asarray(oriented(GLL_EDGE))
    for k in range(4):
        point_index = (partner[k][:, None] * 16 + jnp.take(point_table, edge_codes[k], axis=0)).reshape(-1).astype(jnp.int32)
        numerator = numerator.at[:, :, :, GLL_EDGE[k]].add(jnp.take(flat_weighted, point_index, axis=2).reshape(FIELDS, LEV, ELEMS, 4))
        denominator = denominator.at[:, GLL_EDGE[k]].add(jnp.take(flat_mass, point_index).reshape(ELEMS, 4))
    gll_tendency = (numerator / denominator).reshape(FIELDS, LEV, 16 * ELEMS)
    return (new_state, gll_tendency)
```

```python
import functools
import math

import jax
import jax.numpy as jnp
import numpy as np
from jax import lax
from jax.experimental import pallas as pl
from jax.experimental.pallas import tpu as pltpu
from jax.sharding import PartitionSpec as P

NSUB = 2
PER_TIME = 10.0
CELL_EDGE = [[0, 1], [1, 3], [2, 3], [0, 2]]
MESH = pl.DeviceIdType.MESH
F32 = jnp.float32
BF16 = jnp.bfloat16
NOWHERE = -100000
NN = (((1,), (0,)), ((), ()))
NT = (((1,), (1,)), ((), ()))
TN = (((0,), (0,)), ((), ()))


def lagrange(q, z):
    centres = [-1.5, -0.5, 0.5, 1.5]
    product = 1.0
    for r in range(4):
        if r != q:
            product = product * (z - centres[r]) / (centres[q] - centres[r])
    return product


def linear_weight(j, z):
    return 0.5 - z if j == 0 else 0.5 + z


def remap_matrix():
    gll_nodes = [-1.0, -1.0 / math.sqrt(5.0), 1.0 / math.sqrt(5.0), 1.0]
    matrix = np.zeros((16, 12))
    for b in range(4):
        for a in range(4):
            p = 4 * b + a
            x = gll_nodes[a]
            y = gll_nodes[b]
            for j in range(2):
                for i in range(2):
                    matrix[p, 2 * j + i] += 0.5 * linear_weight(j, y) * lagrange(
                        1 + i, x
                    ) + 0.5 * linear_weight(i, x) * lagrange(1 + j, y)
            for m in range(2):
                matrix[p, 4 + 6 + m] += 0.5 * linear_weight(m, y) * lagrange(0, x)
                matrix[p, 4 + 2 + m] += 0.5 * linear_weight(m, y) * lagrange(3, x)
                matrix[p, 4 + 0 + m] += 0.5 * linear_weight(m, x) * lagrange(0, y)
                matrix[p, 4 + 4 + m] += 0.5 * linear_weight(m, x) * lagrange(3, y)
    return matrix


def iota(shape, dim):
    return lax.broadcasted_iota(jnp.int32, shape, dim)


def dot(a, b, dims):
    return lax.dot_general(
        a, b, dims, precision=lax.Precision.HIGHEST, preferred_element_type=F32
    )


def dot16(a, b, dims):
    return lax.dot_general(a, b, dims, preferred_element_type=F32)


def split(x, parts):
    pieces = []
    for _ in range(parts):
        piece = x.astype(BF16)
        pieces.append(piece)
        x = x - piece.astype(F32)
    return pieces


def spread(v, k, rows):
    return jnp.broadcast_to(v[k : k + 1, :], (rows, v.shape[1]))


def kernel(
    nf,
    nt,
    slots_s,
    codes_s,
    active_s,
    mix_s,
    drift_s,
    cond_s,
    mixz_s,
    mass_ref,
    table_ref,
    crm_hbm,
    state_out,
    gll_out,
    st,
    xs,
    acc0,
    acc1,
    tend,
    w_on,
    snd1t,
    snd1f,
    snd2t,
    snd2f,
    rcv1t,
    rcv1f,
    rcv2t,
    rcv2f,
    load_sem,
    store_sem,
    send_sem,
    recv_sem,
):
    fields, levels, width = st.shape
    flat = fields * levels
    tiles = width // 128
    rows = tend.shape[0]
    fi = lax.axis_index("face")
    ti = lax.axis_index("tile")
    targets = [
        (fi, lax.rem(ti + nt - 1, nt)),
        (fi, lax.rem(ti + 1, nt)),
        (lax.rem(fi + nf - 1, nf), ti),
        (lax.rem(fi + 1, nf), ti),
    ]
    barrier = pltpu.get_barrier_semaphore()
    for target in targets:
        pl.semaphore_signal(barrier, inc=1, device_id=target, device_id_type=MESH)

    load_a = pltpu.make_async_copy(crm_hbm.at[0:3], st.at[0:3], load_sem.at[0])
    load_b = pltpu.make_async_copy(crm_hbm.at[3:6], st.at[3:6], load_sem.at[1])
    load_a.start()
    load_b.start()

    lane8 = iota((8, 128), 1)
    sub8 = iota((8, 128), 0)

    def expanded(source, shift):
        key = sub8 * 32 + (lane8 >> shift)
        out = jnp.full((8, 128), -1, jnp.int32)
        for k in range(4):
            for e in range(8):
                out = jnp.where(key == k * 32 + e, source[k, e], out)
        return out

    def base_of(side):
        return jnp.where(
            side == 1,
            0,
            jnp.where(side == 2, 8, jnp.where(side == 3, 16, jnp.where(side == 4, 20, NOWHERE))),
        )

    def send_row(v, shift):
        side = v >> 3
        own = lane8 >> shift
        rank = jnp.zeros((8, 128), jnp.int32)
        for k in range(4):
            for e in range(8):
                rank = rank + jnp.where((side == (slots_s[k, e] >> 3)) & (own > e), 2, 0)
        return base_of(side) + rank

    def recv_row(v):
        side = v >> 3
        rank = jnp.zeros((8, 128), jnp.int32)
        for k in range(4):
            for e in range(8):
                other = slots_s[k, e]
                rank = rank + jnp.where((side == (other >> 3)) & (v > other), 2, 0)
        return base_of(side) + rank

    v4 = expanded(slots_s, 2)
    row4 = send_row(v4, 2)
    cell = lane8[0:1] & 3
    i24 = iota((24, 128), 0)
    sel1 = jnp.zeros((24, 128), F32)
    for k in range(4):
        first = row4[k : k + 1]
        goal = jnp.where(
            cell == CELL_EDGE[k][0],
            first,
            jnp.where(cell == CELL_EDGE[k][1], first + 1, NOWHERE),
        )
        sel1 = sel1 + jnp.where(i24 == goal, 1.0, 0.0)

    subl = iota((levels, 128), 0)
    upper = jnp.zeros((levels, 128), F32)
    lower = jnp.zeros((levels, 128), F32)
    for l in range(levels - 1):
        k_l = mixz_s[l]
        upper = jnp.where(subl == l, k_l, upper)
        lower = jnp.where(subl == l + 1, k_l, lower)
    centre = 1.0 - upper - lower

    def vertical(a):
        return (
            a * centre
            + upper * pltpu.roll(a, levels - 1, 0)
            + lower * pltpu.roll(a, 1, 0)
        )

    def vertical_change(a):
        return upper * (pltpu.roll(a, levels - 1, 0) - a) + lower * (pltpu.roll(a, 1, 0) - a)

    lane_l = iota((levels, 128), 1)
    east_at = (lane_l & 96) | ((lane_l + 1) & 31)
    west_at = (lane_l & 96) | ((lane_l + 31) & 31)
    group = iota((1, 128), 1) >> 5

    def per_column(source, tile):
        out = source[4 * tile]
        for g in range(1, 4):
            out = jnp.where(group == g, source[4 * tile + g], out)
        return out

    def horizontal_parts(tile):
        mix = per_column(mix_s, tile)
        half = 0.5 * per_column(drift_s, tile)
        return 1.0 - 2.0 * mix, mix - half, mix + half

    def linear(a, parts):
        mid, east, west = parts
        b = (
            a * mid
            + east * jnp.take_along_axis(a, east_at, axis=1)
            + west * jnp.take_along_axis(a, west_at, axis=1)
        )
        return vertical(b)

    def lanes(tile):
        return pl.ds(pl.multiple_of(tile * 128, 128), 128)

    out_lane = iota((256, 128), 1)
    out_row = iota((256, 128), 0)

    def gather_sums(slot, tile):
        x = xs[slot]
        hi, lo = split(x, 2)
        ones = jnp.where(out_lane == 4 * tile + ((out_row & 127) >> 5), 1.0, 0.0).astype(BF16)
        acc1[...] += dot16(jnp.concatenate([hi, lo], axis=1), ones, NN)

    def active_tile(tile, slot):
        parts = horizontal_parts(tile)
        alive = subl < per_column(active_s, tile)
        rate = per_column(cond_s, tile)
        t, qv, ql = (st[f, :, lanes(tile)].astype(F32) for f in range(3))
        for step in range(NSUB):
            t, qv, ql = linear(t, parts), linear(qv, parts), linear(ql, parts)
            sat = 0.5 * jnp.exp(0.3 * t)
            cond = jnp.where(alive, jnp.maximum(rate * (qv - sat), -ql), 0.0)
            qv = qv - cond
            ql = ql + cond
            t = t + 0.5 * cond
            freeze = jnp.where(alive, 0.15 * ql * (1.0 - jnp.tanh(t)), 0.0)
            ql = ql - freeze
            t = t + 0.1 * freeze
            xs[slot, 2 * step * levels : (2 * step + 1) * levels, :] = cond
            xs[slot, (2 * step + 1) * levels : (2 * step + 2) * levels, :] = freeze
        st[0, :, lanes(tile)] = t.astype(BF16)
        st[1, :, lanes(tile)] = qv.astype(BF16)
        st[2, :, lanes(tile)] = ql.astype(BF16)

    acc0[...] = jnp.zeros_like(acc0)
    acc1[...] = jnp.zeros_like(acc1)
    xs[0] = jnp.zeros(xs.shape[1:], F32)
    xs[1] = jnp.zeros(xs.shape[1:], F32)
    tend[flat:rows, :] = jnp.zeros((rows - flat, 128), F32)
    load_a.wait()
    load_b.wait()

    def pair(p, carry):
        two = pl.ds(pl.multiple_of(p * 256, 256), 256)
        ones = jnp.where(out_lane == 8 * p + (out_row >> 5), 1.0, 0.0).astype(BF16)
        start = jnp.concatenate([st[f, :, two].astype(F32) for f in range(fields)], axis=0)
        acc0[...] += dot16(start.astype(BF16), ones, NN)
        gather_sums(2 * p, 2 * p - 2)
        gather_sums(2 * p + 1, 2 * p - 1)
        active_tile(2 * p, 2 * p + 2)
        active_tile(2 * p + 1, 2 * p + 3)
        return carry

    lax.fori_loop(0, tiles // 2, pair, 0)
    gather_sums(tiles, tiles - 2)
    gather_sums(tiles + 1, tiles - 1)

    c1, z1, c2, z2 = (acc1[n * levels : (n + 1) * levels, :] for n in range(4))
    cond_sum = c1 + vertical_change(c1) + c2
    freeze_sum = z1 + vertical_change(z1) + z2
    micro = [
        0.5 * cond_sum + 0.1 * freeze_sum,
        -cond_sum,
        cond_sum - freeze_sum,
        freeze_sum,
        0.0,
        0.0,
    ]
    scale = PER_TIME / 32.0
    for f in range(fields):
        s0 = acc0[f * levels : (f + 1) * levels, :]
        d1 = vertical_change(s0)
        d2 = vertical_change(s0 + d1)
        tend[f * levels : (f + 1) * levels, :] = scale * (d1 + d2 + micro[f])

    all_t = tend[...]
    pick = sel1.astype(BF16)
    message = sum(dot16(pick, piece, NT) for piece in split(all_t, 3))
    snd1t[0] = message[0:8]
    snd1t[1] = message[8:16]
    snd1f[0] = message[16:20]
    snd1f[1] = message[20:24]

    pl.semaphore_wait(barrier, 4)

    def copies(sends, recvs, base):
        out = []
        for o, target in enumerate(targets):
            source, sink = (sends[0], recvs[0]) if o < 2 else (sends[1], recvs[1])
            out.append(
                pltpu.make_async_remote_copy(
                    src_ref=source.at[o % 2],
                    dst_ref=sink.at[1 - o % 2],
                    send_sem=send_sem.at[base + o],
                    recv_sem=recv_sem.at[base + (o ^ 1)],
                    device_id=target,
                    device_id_type=MESH,
                )
            )
        return out

    round1 = copies((snd1t, snd1f), (rcv1t, rcv1f), 0)
    for copy in round1:
        copy.start()

    v = expanded(slots_s, 4)
    q = expanded(codes_s, 4)
    side, pos = v >> 3, v & 7
    their, turned = q >> 1, (q & 1) == 1
    send16, recv16 = send_row(v, 4), recv_row(v)
    point = lane8 & 15
    a_at, b_at = point & 3, point >> 2
    place = jnp.where((sub8 & 1) == 0, a_at, b_at)
    on_edge = (
        ((sub8 == 0) & (b_at == 0))
        | ((sub8 == 1) & (a_at == 3))
        | ((sub8 == 2) & (b_at == 3))
        | ((sub8 == 3) & (a_at == 0))
    )
    there = jnp.where(turned, 3 - place, place)
    cell_a = jnp.where(their == 1, 1, jnp.where(their == 2, 2, 0))
    cell_b = jnp.where(their == 0, 1, jnp.where(their == 3, 2, 3))
    inside = side == 0
    near = [
        jnp.where(inside, 4 * pos + jnp.where(turned, cell_b, cell_a), NOWHERE),
        jnp.where(inside, 4 * pos + jnp.where(turned, cell_a, cell_b), NOWHERE),
    ]
    flip = q & 1
    far = [recv16 + flip, recv16 + 1 - flip]
    send_point = jnp.where(on_edge, 2 * send16 + place, NOWHERE)
    recv_point = jnp.where(on_edge, 2 * recv16 + there, NOWHERE)
    near_point = jnp.where(
        on_edge & inside,
        16 * pos
        + jnp.where((their & 1) == 1, 4 * there, there)
        + jnp.where(their == 1, 3, jnp.where(their == 2, 12, 0)),
        NOWHERE,
    )
    mass = mass_ref[...]
    table = table_ref[...] * mass
    i32 = iota((32, 128), 0)
    i48 = iota((48, 128), 0)
    i128 = iota((128, 128), 0)
    r_on = jnp.zeros((32, 128), F32)
    r_far = jnp.zeros((24, 128), F32)
    sel2 = jnp.zeros((48, 128), F32)
    q_far = jnp.zeros((48, 128), F32)
    q_on = jnp.where(i128 == lane8[0:1], 1.0, 0.0)
    own4 = 4 * (lane8[0:1] >> 4)
    for c in range(4):
        r_on = r_on + jnp.where(i32 == own4 + c, table[c : c + 1], 0.0)
    for k in range(4):
        for m in range(2):
            weight = table[4 + 2 * k + m : 5 + 2 * k + m]
            r_on = r_on + jnp.where(i32 == near[m][k : k + 1], weight, 0.0)
            r_far = r_far + jnp.where(i24 == far[m][k : k + 1], weight, 0.0)
        sel2 = sel2 + jnp.where(i48 == send_point[k : k + 1], 1.0, 0.0)
        q_far = q_far + jnp.where(i48 == recv_point[k : k + 1], 1.0, 0.0)
        q_on = q_on + jnp.where(i128 == near_point[k : k + 1], 1.0, 0.0)

    r_on = jnp.concatenate([r_on, jnp.zeros((96, 128), F32)], axis=0)
    w_on[...] = dot(all_t, r_on, NN)
    w_on[flat : flat + 1, :] = mass
    base2 = dot(sel2, w_on[...], NT)
    through = dot(sel2, r_far, NT)

    def passive(tile, carry):
        parts = horizontal_parts(tile)
        qi = st[3, :, lanes(tile)].astype(F32)
        for step in range(NSUB):
            qi = linear(qi, parts)
            qi = qi + xs[tile + 2, (2 * step + 1) * levels : (2 * step + 2) * levels, :]
        st[3, :, lanes(tile)] = qi.astype(BF16)
        for f in range(4, fields):
            a = st[f, :, lanes(tile)].astype(F32)
            for step in range(NSUB):
                a = linear(a, parts)
            st[f, :, lanes(tile)] = a.astype(BF16)
        return carry

    lax.fori_loop(0, tiles, passive, 0)
    store = pltpu.make_async_copy(st, state_out, store_sem)
    store.start()

    for copy in round1:
        copy.wait_recv()
    halo = jnp.concatenate([rcv1t[0], rcv1t[1], rcv1f[0], rcv1f[1]], axis=0)
    message = base2 + dot(through, halo, NN)
    snd2t[0] = message[0:16]
    snd2t[1] = message[16:32]
    snd2f[0] = message[32:40]
    snd2f[1] = message[40:48]
    round2 = copies((snd2t, snd2f), (rcv2t, rcv2f), 4)
    for copy in round2:
        copy.start()
    weighted = w_on[...] + dot(halo, r_far, TN)
    near_sum = dot(weighted, q_on, NN)
    pick = q_far.astype(BF16)
    pick = jnp.concatenate([pick, pick, pick], axis=0)
    for copy in round2:
        copy.wait_recv()
    halo2 = jnp.concatenate([rcv2t[0], rcv2t[1], rcv2f[0], rcv2f[1]], axis=0)
    pieces = jnp.concatenate(split(halo2, 3), axis=0)
    total = near_sum + dot16(pieces, pick, TN)
    inverse = 1.0 / total[flat : flat + 1, :]
    for f in range(fields):
        gll_out[f] = total[f * levels : (f + 1) * levels, :] * inverse
    for copy in round1 + round2:
        copy.wait_send()
    store.wait()


def local(
    nf,
    nt,
    crm_state,
    active_levels,
    mix_x,
    drift_speed,
    cond_rate,
    mix_z,
    point_mass,
    neighbor_slots,
    edge_codes,
):
    fields, levels, width = crm_state.shape
    flat = fields * levels
    points = point_mass.shape[0]
    wide = 128 * (flat // 128 + 1)
    tiles = width // 128
    matrix = remap_matrix()
    table = np.zeros((16, points), np.float32)
    table[:12] = np.tile(matrix.T, (1, points // 16))
    smem = pl.BlockSpec(memory_space=pltpu.SMEM)
    vmem = pl.BlockSpec(memory_space=pltpu.VMEM)
    hbm = pl.BlockSpec(memory_space=pl.ANY)
    return pl.pallas_call(
        functools.partial(kernel, nf, nt),
        out_shape=(
            jax.ShapeDtypeStruct(crm_state.shape, BF16),
            jax.ShapeDtypeStruct((fields, levels, points), F32),
        ),
        in_specs=[smem] * 7 + [vmem] * 2 + [hbm],
        out_specs=(hbm, vmem),
        scratch_shapes=[
            pltpu.VMEM((fields, levels, width), BF16),
            pltpu.VMEM((tiles + 2, 4 * levels, 128), F32),
            pltpu.VMEM((flat, 128), F32),
            pltpu.VMEM((4 * levels, 128), F32),
            pltpu.VMEM((wide, 128), F32),
            pltpu.VMEM((wide, 128), F32),
            pltpu.VMEM((2, 8, wide), F32),
            pltpu.VMEM((2, 4, wide), F32),
            pltpu.VMEM((2, 16, wide), F32),
            pltpu.VMEM((2, 8, wide), F32),
            pltpu.VMEM((2, 8, wide), F32),
            pltpu.VMEM((2, 4, wide), F32),
            pltpu.VMEM((2, 16, wide), F32),
            pltpu.VMEM((2, 8, wide), F32),
            pltpu.SemaphoreType.DMA((2,)),
            pltpu.SemaphoreType.DMA,
            pltpu.SemaphoreType.DMA((8,)),
            pltpu.SemaphoreType.DMA((8,)),
        ],
        compiler_params=pltpu.CompilerParams(collective_id=0, has_side_effects=True),
    )(
        neighbor_slots,
        edge_codes,
        active_levels,
        mix_x,
        drift_speed,
        cond_rate,
        mix_z,
        point_mass.reshape(1, points),
        jnp.asarray(table),
        crm_state,
    )


def solution(mesh):
    in_specs = (
        P(None, None, ("face", "tile")),
        P(("face", "tile")),
        P(("face", "tile")),
        P(("face", "tile")),
        P(("face", "tile")),
        P(),
        P(("face", "tile")),
        P(None, ("face", "tile")),
        P(None, ("face", "tile")),
    )
    out_specs = (P(None, None, ("face", "tile")), P(None, None, ("face", "tile")))
    body = functools.partial(local, mesh.shape["face"], mesh.shape["tile"])
    return jax.shard_map(body, mesh=mesh, in_specs=in_specs, out_specs=out_specs, check_vma=False)
```

```python
import functools
import math

import jax
import jax.numpy as jnp
import numpy as np
from jax import lax
from jax.experimental import pallas as pl
from jax.experimental.pallas import tpu as pltpu
from jax.sharding import PartitionSpec as P

NSUB = 2
PER_TIME = 10.0
CELL_EDGE = [[0, 1], [1, 3], [2, 3], [0, 2]]
MESH = pl.DeviceIdType.MESH
F32 = jnp.float32
BF16 = jnp.bfloat16
NOWHERE = -100000
NN = (((1,), (0,)), ((), ()))
NT = (((1,), (1,)), ((), ()))
TN = (((0,), (0,)), ((), ()))


def lagrange(q, z):
    centres = [-1.5, -0.5, 0.5, 1.5]
    product = 1.0
    for r in range(4):
        if r != q:
            product = product * (z - centres[r]) / (centres[q] - centres[r])
    return product


def linear_weight(j, z):
    return 0.5 - z if j == 0 else 0.5 + z


def remap_matrix():
    gll_nodes = [-1.0, -1.0 / math.sqrt(5.0), 1.0 / math.sqrt(5.0), 1.0]
    matrix = np.zeros((16, 12))
    for b in range(4):
        for a in range(4):
            p = 4 * b + a
            x = gll_nodes[a]
            y = gll_nodes[b]
            for j in range(2):
                for i in range(2):
                    matrix[p, 2 * j + i] += 0.5 * linear_weight(j, y) * lagrange(
                        1 + i, x
                    ) + 0.5 * linear_weight(i, x) * lagrange(1 + j, y)
            for m in range(2):
                matrix[p, 4 + 6 + m] += 0.5 * linear_weight(m, y) * lagrange(0, x)
                matrix[p, 4 + 2 + m] += 0.5 * linear_weight(m, y) * lagrange(3, x)
                matrix[p, 4 + 0 + m] += 0.5 * linear_weight(m, x) * lagrange(0, y)
                matrix[p, 4 + 4 + m] += 0.5 * linear_weight(m, x) * lagrange(3, y)
    return matrix


def iota(shape, dim):
    return lax.broadcasted_iota(jnp.int32, shape, dim)


def dot(a, b, dims):
    return lax.dot_general(
        a, b, dims, precision=lax.Precision.HIGHEST, preferred_element_type=F32
    )


def dot16(a, b, dims):
    return lax.dot_general(a, b, dims, preferred_element_type=F32)


def split(x, parts):
    pieces = []
    for _ in range(parts):
        piece = x.astype(BF16)
        pieces.append(piece)
        x = x - piece.astype(F32)
    return pieces


def spread(v, k, rows):
    return jnp.broadcast_to(v[k : k + 1, :], (rows, v.shape[1]))


def kernel(
    nf,
    nt,
    slots_hbm,
    codes_hbm,
    active_hbm,
    mix_hbm,
    drift_hbm,
    cond_hbm,
    mixz_hbm,
    mass_hbm,
    table_hbm,
    crm_hbm,
    state_out,
    gll_out,
    slots_s,
    codes_s,
    active_s,
    mix_s,
    drift_s,
    cond_s,
    mixz_s,
    mass_ref,
    table_ref,
    st,
    bs,
    cf,
    ones,
    xs,
    acc0,
    acc1,
    tend,
    w_on,
    snd1t,
    snd1f,
    snd2t,
    snd2f,
    rcv1t,
    rcv1f,
    rcv2t,
    rcv2f,
    load_sem,
    small_sem,
    send_sem,
    recv_sem,
):
    fields, levels, width = st.shape
    flat = fields * levels
    tiles = width // 128
    rows = tend.shape[0]
    fi = lax.axis_index("face")
    ti = lax.axis_index("tile")
    targets = [
        (fi, lax.rem(ti + nt - 1, nt)),
        (fi, lax.rem(ti + 1, nt)),
        (lax.rem(fi + nf - 1, nf), ti),
        (lax.rem(fi + 1, nf), ti),
    ]
    load_a = pltpu.make_async_copy(crm_hbm.at[0:3], st.at[0:3], load_sem.at[0])
    load_b = pltpu.make_async_copy(crm_hbm.at[3:6], st.at[3:6], load_sem.at[1])
    load_a.start()
    smalls = []
    for n, (source, sink) in enumerate(
        (
            (mixz_hbm, mixz_s),
            (mix_hbm, mix_s),
            (drift_hbm, drift_s),
            (cond_hbm, cond_s),
            (active_hbm, active_s),
            (slots_hbm, slots_s),
            (codes_hbm, codes_s),
            (mass_hbm, mass_ref),
            (table_hbm, table_ref),
        )
    ):
        smalls.append(pltpu.make_async_copy(source, sink, small_sem.at[n]))
        smalls[-1].start()
    load_b.start()
    barrier = pltpu.get_barrier_semaphore()
    for target in targets:
        pl.semaphore_signal(barrier, inc=1, device_id=target, device_id_type=MESH)

    lane8 = iota((8, 128), 1)
    sub8 = iota((8, 128), 0)

    def expanded(source, shift):
        key = sub8 * 32 + (lane8 >> shift)
        out = jnp.full((8, 128), -1, jnp.int32)
        for k in range(4):
            for e in range(8):
                out = jnp.where(key == k * 32 + e, source[k, e], out)
        return out

    def base_of(side):
        return jnp.where(
            side == 1,
            0,
            jnp.where(side == 2, 8, jnp.where(side == 3, 16, jnp.where(side == 4, 20, NOWHERE))),
        )

    def send_row(v, shift):
        side = v >> 3
        own = lane8 >> shift
        rank = jnp.zeros((8, 128), jnp.int32)
        for k in range(4):
            for e in range(8):
                rank = rank + jnp.where((side == (slots_s[k, e] >> 3)) & (own > e), 2, 0)
        return base_of(side) + rank

    def recv_row(v):
        side = v >> 3
        rank = jnp.zeros((8, 128), jnp.int32)
        for k in range(4):
            for e in range(8):
                other = slots_s[k, e]
                rank = rank + jnp.where((side == (other >> 3)) & (v > other), 2, 0)
        return base_of(side) + rank

    lane_r = iota((256, 128), 0) >> 5
    lane_n = iota((256, 128), 1)
    for p in range(width // 256):
        ones[256 * p : 256 * (p + 1), :] = jnp.where(lane_n == lane_r + 8 * p, 1.0, 0.0)
    acc0[...] = jnp.zeros_like(acc0)
    acc1[...] = jnp.zeros_like(acc1)
    xs[0] = jnp.zeros(xs.shape[1:], F32)
    xs[1] = jnp.zeros(xs.shape[1:], F32)
    tend[flat:rows, :] = jnp.zeros((rows - flat, 128), F32)
    blank = jnp.zeros((8, 128), F32)
    for n in range(bs.shape[0]):
        bs[n, 0:8, :] = blank
        bs[n, levels + 8 : levels + 16, :] = blank

    for copy in smalls:
        copy.wait()

    chunks = levels // 8
    for r in range(chunks):
        upper, lower = blank, blank
        for s in range(8):
            l = 8 * r + s
            if l < levels - 1:
                upper = jnp.where(sub8 == s, mixz_s[l], upper)
            if l > 0:
                lower = jnp.where(sub8 == s, mixz_s[l - 1], lower)
        cf[0, 8 * r : 8 * r + 8, :] = upper
        cf[1, 8 * r : 8 * r + 8, :] = lower
        cf[2, 8 * r : 8 * r + 8, :] = 1.0 - upper - lower

    v4 = expanded(slots_s, 2)
    row4 = send_row(v4, 2)
    cell = lane8[0:1] & 3
    i24 = iota((24, 128), 0)
    sel1 = jnp.zeros((24, 128), F32)
    for k in range(4):
        first = row4[k : k + 1]
        goal = jnp.where(
            cell == CELL_EDGE[k][0],
            first,
            jnp.where(cell == CELL_EDGE[k][1], first + 1, NOWHERE),
        )
        sel1 = sel1 + jnp.where(i24 == goal, 1.0, 0.0)

    def part(r, shift=0):
        return slice(8 * r + shift, 8 * r + 8 + shift)

    def vertical(buffer, r):
        return (
            cf[2, part(r), :] * buffer[part(r, 8), :]
            + cf[0, part(r), :] * buffer[part(r, 9), :]
            + cf[1, part(r), :] * buffer[part(r, 7), :]
        )

    def vertical_change(a):
        upper, lower = cf[0], cf[1]
        return upper * (pltpu.roll(a, levels - 1, 0) - a) + lower * (pltpu.roll(a, 1, 0) - a)

    east_at = (lane8 & 96) | ((lane8 + 1) & 31)
    west_at = (lane8 & 96) | ((lane8 + 31) & 31)
    group = lane8 >> 5

    def per_column(source, tile):
        out = jnp.full((8, 128), source[4 * tile])
        for g in range(1, 4):
            out = jnp.where(group == g, source[4 * tile + g], out)
        return out

    def horizontal_parts(tile):
        mix = per_column(mix_s, tile)
        half = 0.5 * per_column(drift_s, tile)
        return 1.0 - 2.0 * mix, mix - half, mix + half

    def horizontal(a, parts):
        mid, east, west = parts
        return (
            a * mid
            + east * jnp.take_along_axis(a, east_at, axis=1)
            + west * jnp.take_along_axis(a, west_at, axis=1)
        )

    def lanes(tile):
        return pl.ds(pl.multiple_of(tile * 128, 128), 128)

    def gather_sums(slot, tile):
        x = xs[slot]
        head = x.astype(BF16).astype(F32)
        rest = x - head
        pick = ones[pl.ds(pl.multiple_of(tile * 128, 128), 128), :]
        acc1[...] += dot16(
            jnp.concatenate([head, rest], axis=1), jnp.concatenate([pick, pick], axis=0), NN
        )

    def active_tile(tile, slot, lot):
        parts = horizontal_parts(tile)
        limit = per_column(active_s, tile)
        rate = per_column(cond_s, tile)
        for r in range(chunks):
            for f in range(3):
                a = st[f, part(r), lanes(tile)].astype(F32)
                bs[lot + f, part(r, 8), :] = horizontal(a, parts)
        for step in range(NSUB):
            for r in range(chunks):
                t, qv, ql = (vertical(bs.at[lot + 3 * step + f], r) for f in range(3))
                alive = sub8 + 8 * r < limit
                sat = 0.5 * jnp.exp(0.3 * t)
                cond = jnp.where(alive, jnp.maximum(rate * (qv - sat), -ql), 0.0)
                qv = qv - cond
                ql = ql + cond
                t = t + 0.5 * cond
                freeze = jnp.where(alive, 0.15 * ql * (1.0 - jnp.tanh(t)), 0.0)
                ql = ql - freeze
                t = t + 0.1 * freeze
                at = 2 * step * levels + 8 * r
                xs[slot, at : at + 8, :] = cond
                xs[slot, at + levels : at + levels + 8, :] = freeze
                for f, a in enumerate((t, qv, ql)):
                    if step + 1 < NSUB:
                        bs[lot + 3 * (step + 1) + f, part(r, 8), :] = horizontal(a, parts)
                    else:
                        st[f, part(r), lanes(tile)] = a.astype(BF16)

    load_a.wait()
    load_b.wait()

    def pair(p, carry):
        two = pl.ds(pl.multiple_of(p * 256, 256), 256)
        start = jnp.concatenate([st[f, :, two].astype(F32) for f in range(fields)], axis=0)
        acc0[...] += dot16(start, ones[two, :], NN)
        gather_sums(2 * p, max(2 * p - 2, 0))
        gather_sums(2 * p + 1, max(2 * p - 1, 0))
        active_tile(2 * p, 2 * p + 2, 0)
        active_tile(2 * p + 1, 2 * p + 3, 6)
        return carry

    for p in range(tiles // 2):
        pair(p, 0)
    gather_sums(tiles, tiles - 2)
    gather_sums(tiles + 1, tiles - 1)

    c1, z1, c2, z2 = (acc1[n * levels : (n + 1) * levels, :] for n in range(4))
    cond_sum = c1 + vertical_change(c1) + c2
    freeze_sum = z1 + vertical_change(z1) + z2
    micro = [
        0.5 * cond_sum + 0.1 * freeze_sum,
        -cond_sum,
        cond_sum - freeze_sum,
        freeze_sum,
        0.0,
        0.0,
    ]
    scale = PER_TIME / 32.0
    for f in range(fields):
        s0 = acc0[f * levels : (f + 1) * levels, :]
        d1 = vertical_change(s0)
        d2 = vertical_change(s0 + d1)
        tend[f * levels : (f + 1) * levels, :] = scale * (d1 + d2 + micro[f])

    all_t = tend[...]
    pick = sel1.astype(BF16)
    message = sum(dot16(pick, piece, NT) for piece in split(all_t, 3))
    snd1t[0] = message[0:8]
    snd1t[1] = message[8:16]
    snd1f[0] = message[16:20]
    snd1f[1] = message[20:24]

    pl.semaphore_wait(barrier, 4)

    def copies(sends, recvs, base):
        out = []
        for o, target in enumerate(targets):
            source, sink = (sends[0], recvs[0]) if o < 2 else (sends[1], recvs[1])
            out.append(
                pltpu.make_async_remote_copy(
                    src_ref=source.at[o % 2],
                    dst_ref=sink.at[1 - o % 2],
                    send_sem=send_sem.at[base + o],
                    recv_sem=recv_sem.at[base + (o ^ 1)],
                    device_id=target,
                    device_id_type=MESH,
                )
            )
        return out

    round1 = copies((snd1t, snd1f), (rcv1t, rcv1f), 0)
    for copy in round1:
        copy.start()

    v = expanded(slots_s, 4)
    q = expanded(codes_s, 4)
    side, pos = v >> 3, v & 7
    their, turned = q >> 1, (q & 1) == 1
    send16, recv16 = send_row(v, 4), recv_row(v)
    point = lane8 & 15
    a_at, b_at = point & 3, point >> 2
    place = jnp.where((sub8 & 1) == 0, a_at, b_at)
    on_edge = (
        ((sub8 == 0) & (b_at == 0))
        | ((sub8 == 1) & (a_at == 3))
        | ((sub8 == 2) & (b_at == 3))
        | ((sub8 == 3) & (a_at == 0))
    )
    there = jnp.where(turned, 3 - place, place)
    cell_a = jnp.where(their == 1, 1, jnp.where(their == 2, 2, 0))
    cell_b = jnp.where(their == 0, 1, jnp.where(their == 3, 2, 3))
    inside = side == 0
    near = [
        jnp.where(inside, 4 * pos + jnp.where(turned, cell_b, cell_a), NOWHERE),
        jnp.where(inside, 4 * pos + jnp.where(turned, cell_a, cell_b), NOWHERE),
    ]
    flip = q & 1
    far = [recv16 + flip, recv16 + 1 - flip]
    send_point = jnp.where(on_edge, 2 * send16 + place, NOWHERE)
    recv_point = jnp.where(on_edge, 2 * recv16 + there, NOWHERE)
    near_point = jnp.where(
        on_edge & inside,
        16 * pos
        + jnp.where((their & 1) == 1, 4 * there, there)
        + jnp.where(their == 1, 3, jnp.where(their == 2, 12, 0)),
        NOWHERE,
    )
    mass = mass_ref[...]
    table = table_ref[...] * mass
    i32 = iota((32, 128), 0)
    i48 = iota((48, 128), 0)
    i128 = iota((128, 128), 0)
    r_on = jnp.zeros((32, 128), F32)
    r_far = jnp.zeros((24, 128), F32)
    sel2 = jnp.zeros((48, 128), F32)
    q_far = jnp.zeros((48, 128), F32)
    q_on = jnp.where(i128 == lane8[0:1], 1.0, 0.0)
    own4 = 4 * (lane8[0:1] >> 4)
    for c in range(4):
        r_on = r_on + jnp.where(i32 == own4 + c, table[c : c + 1], 0.0)
    for k in range(4):
        for m in range(2):
            weight = table[4 + 2 * k + m : 5 + 2 * k + m]
            r_on = r_on + jnp.where(i32 == near[m][k : k + 1], weight, 0.0)
            r_far = r_far + jnp.where(i24 == far[m][k : k + 1], weight, 0.0)
        sel2 = sel2 + jnp.where(i48 == send_point[k : k + 1], 1.0, 0.0)
        q_far = q_far + jnp.where(i48 == recv_point[k : k + 1], 1.0, 0.0)
        q_on = q_on + jnp.where(i128 == near_point[k : k + 1], 1.0, 0.0)

    r_on = jnp.concatenate([r_on, jnp.zeros((96, 128), F32)], axis=0)
    w_on[...] = dot(all_t, r_on, NN)
    w_on[flat : flat + 1, :] = mass
    base2 = dot(sel2, w_on[...], NT)
    through = dot(sel2, r_far, NT)

    for copy in round1:
        copy.wait_recv()
    halo = jnp.concatenate([rcv1t[0], rcv1t[1], rcv1f[0], rcv1f[1]], axis=0)
    message = base2 + dot(through, halo, NN)
    snd2t[0] = message[0:16]
    snd2t[1] = message[16:32]
    snd2f[0] = message[32:40]
    snd2f[1] = message[40:48]
    round2 = copies((snd2t, snd2f), (rcv2t, rcv2f), 4)
    for copy in round2:
        copy.start()
    def passive(tile, carry):
        parts = horizontal_parts(tile)
        for r in range(chunks):
            for f in range(3):
                a = st[3 + f, part(r), lanes(tile)].astype(F32)
                bs[f, part(r, 8), :] = horizontal(a, parts)
        for step in range(NSUB):
            for r in range(chunks):
                for f in range(3):
                    a = vertical(bs.at[3 * step + f], r)
                    if f == 0:
                        at = (2 * step + 1) * levels + 8 * r
                        a = a + xs[tile + 2, at : at + 8, :]
                    if step + 1 < NSUB:
                        bs[3 * (step + 1) + f, part(r, 8), :] = horizontal(a, parts)
                    else:
                        state_out[3 + f, part(r), lanes(tile)] = a.astype(BF16)
        for f in range(3):
            state_out[f, :, lanes(tile)] = st[f, :, lanes(tile)]
        return carry

    lax.fori_loop(0, tiles, passive, 0)
    weighted = w_on[...] + dot(halo, r_far, TN)
    near_sum = dot(weighted, q_on, NN)
    pick = q_far.astype(BF16)
    pick = jnp.concatenate([pick, pick, pick], axis=0)
    for copy in round2:
        copy.wait_recv()
    halo2 = jnp.concatenate([rcv2t[0], rcv2t[1], rcv2f[0], rcv2f[1]], axis=0)
    pieces = jnp.concatenate(split(halo2, 3), axis=0)
    total = near_sum + dot16(pieces, pick, TN)
    inverse = 1.0 / total[flat : flat + 1, :]
    for f in range(fields):
        gll_out[f] = total[f * levels : (f + 1) * levels, :] * inverse
    for copy in round1 + round2:
        copy.wait_send()


def local(
    nf,
    nt,
    crm_state,
    active_levels,
    mix_x,
    drift_speed,
    cond_rate,
    mix_z,
    point_mass,
    neighbor_slots,
    edge_codes,
):
    fields, levels, width = crm_state.shape
    flat = fields * levels
    points = point_mass.shape[0]
    wide = 128 * (flat // 128 + 1)
    tiles = width // 128
    matrix = remap_matrix()
    table = np.zeros((16, points), np.float32)
    table[:12] = np.tile(matrix.T, (1, points // 16))
    vmem = pl.BlockSpec(memory_space=pltpu.VMEM)
    hbm = pl.BlockSpec(memory_space=pltpu.HBM)
    return pl.pallas_call(
        functools.partial(kernel, nf, nt),
        out_shape=(
            jax.ShapeDtypeStruct(crm_state.shape, BF16),
            jax.ShapeDtypeStruct((fields, levels, points), F32),
        ),
        in_specs=[hbm] * 10,
        out_specs=(vmem, vmem),
        scratch_shapes=[
            pltpu.SMEM(neighbor_slots.shape, jnp.int32),
            pltpu.SMEM(edge_codes.shape, jnp.int32),
            pltpu.SMEM(active_levels.shape, jnp.int32),
            pltpu.SMEM(mix_x.shape, F32),
            pltpu.SMEM(drift_speed.shape, F32),
            pltpu.SMEM(cond_rate.shape, F32),
            pltpu.SMEM(mix_z.shape, F32),
            pltpu.VMEM((1, points), F32),
            pltpu.VMEM(table.shape, F32),
            pltpu.VMEM((fields, levels, width), BF16),
            pltpu.VMEM((12, levels + 16, 128), F32),
            pltpu.VMEM((3, levels, 128), F32),
            pltpu.VMEM((width, 128), F32),
            pltpu.VMEM((tiles + 2, 4 * levels, 128), F32),
            pltpu.VMEM((flat, 128), F32),
            pltpu.VMEM((4 * levels, 128), F32),
            pltpu.VMEM((wide, 128), F32),
            pltpu.VMEM((wide, 128), F32),
            pltpu.VMEM((2, 8, wide), F32),
            pltpu.VMEM((2, 4, wide), F32),
            pltpu.VMEM((2, 16, wide), F32),
            pltpu.VMEM((2, 8, wide), F32),
            pltpu.VMEM((2, 8, wide), F32),
            pltpu.VMEM((2, 4, wide), F32),
            pltpu.VMEM((2, 16, wide), F32),
            pltpu.VMEM((2, 8, wide), F32),
            pltpu.SemaphoreType.DMA((2,)),
            pltpu.SemaphoreType.DMA((9,)),
            pltpu.SemaphoreType.DMA((8,)),
            pltpu.SemaphoreType.DMA((8,)),
        ],
        compiler_params=pltpu.CompilerParams(collective_id=0, has_side_effects=True, vmem_limit_bytes=40 << 20),
    )(
        *(
            pltpu.with_memory_space_constraint(x, pltpu.HBM)
            for x in (
                neighbor_slots,
                edge_codes,
                active_levels,
                mix_x,
                drift_speed,
                cond_rate,
                mix_z,
                point_mass.reshape(1, points),
                jnp.asarray(table),
                crm_state,
            )
        )
    )


def solution(mesh):
    in_specs = (
        P(None, None, ("face", "tile")),
        P(("face", "tile")),
        P(("face", "tile")),
        P(("face", "tile")),
        P(("face", "tile")),
        P(),
        P(("face", "tile")),
        P(None, ("face", "tile")),
        P(None, ("face", "tile")),
    )
    out_specs = (P(None, None, ("face", "tile")), P(None, None, ("face", "tile")))
    body = functools.partial(local, mesh.shape["face"], mesh.shape["tile"])
    return jax.shard_map(body, mesh=mesh, in_specs=in_specs, out_specs=out_specs, check_vma=False)
```

```python
import functools
import math

import jax
import jax.numpy as jnp
import numpy as np
from jax import lax
from jax.experimental import pallas as pl
from jax.experimental.pallas import tpu as pltpu
from jax.sharding import PartitionSpec as P

NSUB = 2
PER_TIME = 10.0
CELL_EDGE = [[0, 1], [1, 3], [2, 3], [0, 2]]
MESH = pl.DeviceIdType.MESH
F32 = jnp.float32
BF16 = jnp.bfloat16
NOWHERE = -100000
NN = (((1,), (0,)), ((), ()))
NT = (((1,), (1,)), ((), ()))
TN = (((0,), (0,)), ((), ()))


def lagrange(q, z):
    centres = [-1.5, -0.5, 0.5, 1.5]
    product = 1.0
    for r in range(4):
        if r != q:
            product = product * (z - centres[r]) / (centres[q] - centres[r])
    return product


def linear_weight(j, z):
    return 0.5 - z if j == 0 else 0.5 + z


def remap_matrix():
    gll_nodes = [-1.0, -1.0 / math.sqrt(5.0), 1.0 / math.sqrt(5.0), 1.0]
    matrix = np.zeros((16, 12))
    for b in range(4):
        for a in range(4):
            p = 4 * b + a
            x = gll_nodes[a]
            y = gll_nodes[b]
            for j in range(2):
                for i in range(2):
                    matrix[p, 2 * j + i] += 0.5 * linear_weight(j, y) * lagrange(
                        1 + i, x
                    ) + 0.5 * linear_weight(i, x) * lagrange(1 + j, y)
            for m in range(2):
                matrix[p, 4 + 6 + m] += 0.5 * linear_weight(m, y) * lagrange(0, x)
                matrix[p, 4 + 2 + m] += 0.5 * linear_weight(m, y) * lagrange(3, x)
                matrix[p, 4 + 0 + m] += 0.5 * linear_weight(m, x) * lagrange(0, y)
                matrix[p, 4 + 4 + m] += 0.5 * linear_weight(m, x) * lagrange(3, y)
    return matrix


def iota(shape, dim):
    return lax.broadcasted_iota(jnp.int32, shape, dim)


def dot(a, b, dims):
    return lax.dot_general(
        a, b, dims, precision=lax.Precision.HIGHEST, preferred_element_type=F32
    )


def dot16(a, b, dims):
    return lax.dot_general(a, b, dims, preferred_element_type=F32)


def halves(x):
    head = x.astype(BF16).astype(F32)
    return head, x - head


def kernel(
    nf,
    nt,
    slots_hbm,
    codes_hbm,
    active_hbm,
    mix_hbm,
    drift_hbm,
    cond_hbm,
    mixz_hbm,
    mass_hbm,
    table_hbm,
    crm_hbm,
    state_out,
    gll_out,
    slots_s,
    codes_s,
    active_s,
    mix_s,
    drift_s,
    cond_s,
    mixz_s,
    mass_ref,
    table_ref,
    st,
    bs,
    cf,
    ones,
    xs,
    acc0,
    acc1,
    tend,
    w_on,
    snd1t,
    snd1f,
    snd2t,
    snd2f,
    rcv1t,
    rcv1f,
    rcv2t,
    rcv2f,
    load_sem,
    small_sem,
    send_sem,
    recv_sem,
):
    fields, levels, width = st.shape
    flat = fields * levels
    tiles = width // 128
    rows = tend.shape[0]
    fi = lax.axis_index("face")
    ti = lax.axis_index("tile")
    targets = [
        (fi, lax.rem(ti + nt - 1, nt)),
        (fi, lax.rem(ti + 1, nt)),
        (lax.rem(fi + nf - 1, nf), ti),
        (lax.rem(fi + 1, nf), ti),
    ]
    load_a = pltpu.make_async_copy(crm_hbm.at[0:3], st.at[0:3], load_sem.at[0])
    load_b = pltpu.make_async_copy(crm_hbm.at[3:6], st.at[3:6], load_sem.at[1])
    load_a.start()
    smalls = []
    for n, (source, sink) in enumerate(
        (
            (mixz_hbm, mixz_s),
            (mix_hbm, mix_s),
            (drift_hbm, drift_s),
            (cond_hbm, cond_s),
            (active_hbm, active_s),
            (slots_hbm, slots_s),
            (codes_hbm, codes_s),
            (mass_hbm, mass_ref),
            (table_hbm, table_ref),
        )
    ):
        smalls.append(pltpu.make_async_copy(source, sink, small_sem.at[n]))
        smalls[-1].start()
    load_b.start()
    barrier = pltpu.get_barrier_semaphore()
    for target in targets:
        pl.semaphore_signal(barrier, inc=1, device_id=target, device_id_type=MESH)

    lane8 = iota((8, 128), 1)
    sub8 = iota((8, 128), 0)

    own16 = lane8 >> 4
    own4 = (lane8 & 31) >> 2

    def expanded(source, own):
        key = sub8 * 32 + own
        out = jnp.full((8, 128), -1, jnp.int32)
        for k in range(4):
            for e in range(8):
                out = jnp.where(key == k * 32 + e, source[k, e], out)
        return out

    def base_of(side):
        return jnp.where(
            side == 1,
            0,
            jnp.where(side == 2, 8, jnp.where(side == 3, 16, jnp.where(side == 4, 20, NOWHERE))),
        )

    def send_row(v, own):
        side = v >> 3
        rank = jnp.zeros((8, 128), jnp.int32)
        for k in range(4):
            for e in range(8):
                rank = rank + jnp.where((side == (slots_s[k, e] >> 3)) & (own > e), 2, 0)
        return base_of(side) + rank

    def recv_row(v):
        side = v >> 3
        rank = jnp.zeros((8, 128), jnp.int32)
        for k in range(4):
            for e in range(8):
                other = slots_s[k, e]
                rank = rank + jnp.where((side == (other >> 3)) & (v > other), 2, 0)
        return base_of(side) + rank

    lane_r = iota((256, 128), 0) >> 5
    lane_n = iota((256, 128), 1) & 31
    for p in range(width // 256):
        ones[256 * p : 256 * (p + 1), :] = jnp.where(lane_n == lane_r + 8 * p, 1.0, 0.0)
    acc0[...] = jnp.zeros_like(acc0)
    acc1[...] = jnp.zeros_like(acc1)
    xs[0] = jnp.zeros(xs.shape[1:], F32)
    xs[1] = jnp.zeros(xs.shape[1:], F32)
    tend[flat:rows, :] = jnp.zeros((rows - flat, 128), F32)
    blank = jnp.zeros((8, 128), F32)
    for n in range(bs.shape[0]):
        bs[n, 0:8, :] = blank
        bs[n, levels + 8 : levels + 16, :] = blank
    for n in range(cf.shape[0]):
        cf[n, 0:8, :] = blank
        cf[n, levels + 8 : levels + 16, :] = blank

    for copy in smalls:
        copy.wait()

    chunks = levels // 8
    for r in range(chunks):
        upper, lower = blank, blank
        for s in range(8):
            l = 8 * r + s
            if l < levels - 1:
                upper = jnp.where(sub8 == s, mixz_s[l], upper)
            if l > 0:
                lower = jnp.where(sub8 == s, mixz_s[l - 1], lower)
        cf[0, 8 * r + 8 : 8 * r + 16, :] = upper
        cf[1, 8 * r + 8 : 8 * r + 16, :] = lower
        cf[2, 8 * r + 8 : 8 * r + 16, :] = 1.0 - upper - lower

    v4 = expanded(slots_s, own4)
    row4 = jnp.where((lane8 & 32) == 0, send_row(v4, own4), NOWHERE)
    cell = lane8[0:1] & 3
    i24 = iota((24, 128), 0)
    sel1 = jnp.zeros((24, 128), F32)
    for k in range(4):
        first = row4[k : k + 1]
        goal = jnp.where(
            cell == CELL_EDGE[k][0],
            first,
            jnp.where(cell == CELL_EDGE[k][1], first + 1, NOWHERE),
        )
        sel1 = sel1 + jnp.where(i24 == goal, 1.0, 0.0)

    def part(r, shift=0):
        return slice(8 * r + shift, 8 * r + 8 + shift)

    def vertical(buffer, r):
        return (
            cf[2, part(r, 8), :] * buffer[part(r, 8), :]
            + cf[0, part(r, 8), :] * buffer[part(r, 9), :]
            + cf[1, part(r, 8), :] * buffer[part(r, 7), :]
        )

    east_at = (lane8 & 96) | ((lane8 + 1) & 31)
    west_at = (lane8 & 96) | ((lane8 + 31) & 31)
    group = lane8 >> 5

    def per_column(source, tile):
        out = jnp.full((8, 128), source[4 * tile])
        for g in range(1, 4):
            out = jnp.where(group == g, source[4 * tile + g], out)
        return out

    def horizontal_parts(tile):
        mix = per_column(mix_s, tile)
        half = 0.5 * per_column(drift_s, tile)
        return 1.0 - 2.0 * mix, mix - half, mix + half

    def horizontal(a, parts):
        mid, east, west = parts
        return (
            a * mid
            + east * jnp.take_along_axis(a, east_at, axis=1)
            + west * jnp.take_along_axis(a, west_at, axis=1)
        )

    def lanes(tile):
        return pl.ds(pl.multiple_of(tile * 128, 128), 128)

    def gather_sums(slot, tile):
        x = xs[slot]
        head = x.astype(BF16).astype(F32)
        rest = x - head
        pick = ones[pl.ds(pl.multiple_of(tile * 128, 128), 128), :]
        sums = dot16(
            jnp.concatenate([head, rest], axis=1), jnp.concatenate([pick, pick], axis=0), NN
        )
        for n in range(4):
            acc1[n, 8 : levels + 8, :] += sums[n * levels : (n + 1) * levels]

    def active_tile(tile, slot, lot):
        parts = horizontal_parts(tile)
        limit = per_column(active_s, tile)
        rate = per_column(cond_s, tile)
        for r in range(chunks):
            for f in range(3):
                a = st[f, part(r), lanes(tile)].astype(F32)
                bs[lot + f, part(r, 8), :] = horizontal(a, parts)
        for step in range(NSUB):
            for r in range(chunks):
                t, qv, ql = (vertical(bs.at[lot + 3 * step + f], r) for f in range(3))
                alive = sub8 + 8 * r < limit
                sat = 0.5 * jnp.exp(0.3 * t)
                cond = jnp.where(alive, jnp.maximum(rate * (qv - sat), -ql), 0.0)
                qv = qv - cond
                ql = ql + cond
                t = t + 0.5 * cond
                freeze = jnp.where(alive, 0.15 * ql * (1.0 - jnp.tanh(t)), 0.0)
                ql = ql - freeze
                t = t + 0.1 * freeze
                at = 2 * step * levels + 8 * r
                xs[slot, at : at + 8, :] = cond
                xs[slot, at + levels : at + levels + 8, :] = freeze
                for f, a in enumerate((t, qv, ql)):
                    if step + 1 < NSUB:
                        bs[lot + 3 * (step + 1) + f, part(r, 8), :] = horizontal(a, parts)
                    else:
                        st[f, part(r), lanes(tile)] = a.astype(BF16)

    load_a.wait()
    load_b.wait()

    def pair(p, carry):
        two = pl.ds(pl.multiple_of(p * 256, 256), 256)
        start = jnp.concatenate([st[f, :, two].astype(F32) for f in range(fields)], axis=0)
        sums = dot16(start, ones[two, :], NN)
        for f in range(fields):
            acc0[f, 8 : levels + 8, :] += sums[f * levels : (f + 1) * levels]
        gather_sums(2 * p, max(2 * p - 2, 0))
        gather_sums(2 * p + 1, max(2 * p - 1, 0))
        active_tile(2 * p, 2 * p + 2, 0)
        active_tile(2 * p + 1, 2 * p + 3, 6)
        return carry

    for p in range(tiles // 2):
        pair(p, 0)
    gather_sums(tiles, tiles - 2)
    gather_sums(tiles + 1, tiles - 1)

    scale = PER_TIME / 32.0
    for r in range(chunks):
        upper, lower, middle = (cf[n, part(r, 8), :] for n in range(3))
        two_up = scale * upper * cf[0, part(r, 9), :]
        one_up = scale * upper * (middle + cf[2, part(r, 9), :])
        one_down = scale * lower * (middle + cf[2, part(r, 7), :])
        two_down = scale * lower * cf[1, part(r, 7), :]
        same = scale * (upper * upper + lower * lower + middle * middle - 1.0)
        cond_sum = scale * (vertical(acc1.at[0], r) + acc1[2, part(r, 8), :])
        freeze_sum = scale * (vertical(acc1.at[1], r) + acc1[3, part(r, 8), :])
        micro = [
            0.5 * cond_sum + 0.1 * freeze_sum,
            -cond_sum,
            cond_sum - freeze_sum,
            freeze_sum,
        ]
        for f in range(fields):
            d = (
                same * acc0[f, part(r, 8), :]
                + (one_up * acc0[f, part(r, 9), :] + one_down * acc0[f, part(r, 7), :])
                + (two_up * acc0[f, part(r, 10), :] + two_down * acc0[f, part(r, 6), :])
            )
            if f < len(micro):
                d = d + micro[f]
            at = f * levels + 8 * r
            tend[at : at + 8, :] = d

    head, rest = halves(tend[...])
    wide_group = iota((rows, 128), 1) >> 5
    pieces_t = jnp.where(wide_group < 2, head, jnp.where(wide_group == 2, rest, 0.0)).astype(BF16)
    message = dot16(sel1.astype(BF16), pieces_t, NT)
    snd1t[0] = message[0:8]
    snd1t[1] = message[8:16]
    snd1f[0] = message[16:20]
    snd1f[1] = message[20:24]

    pl.semaphore_wait(barrier, 4)

    def copies(sends, recvs, base):
        out = []
        for o, target in enumerate(targets):
            source, sink = (sends[0], recvs[0]) if o < 2 else (sends[1], recvs[1])
            out.append(
                pltpu.make_async_remote_copy(
                    src_ref=source.at[o % 2],
                    dst_ref=sink.at[1 - o % 2],
                    send_sem=send_sem.at[base + o],
                    recv_sem=recv_sem.at[base + (o ^ 1)],
                    device_id=target,
                    device_id_type=MESH,
                )
            )
        return out

    round1 = copies((snd1t, snd1f), (rcv1t, rcv1f), 0)
    for copy in round1:
        copy.start()

    v = expanded(slots_s, own16)
    q = expanded(codes_s, own16)
    side, pos = v >> 3, v & 7
    their, turned = q >> 1, (q & 1) == 1
    send16, recv16 = send_row(v, own16), recv_row(v)
    point = lane8 & 15
    a_at, b_at = point & 3, point >> 2
    place = jnp.where((sub8 & 1) == 0, a_at, b_at)
    on_edge = (
        ((sub8 == 0) & (b_at == 0))
        | ((sub8 == 1) & (a_at == 3))
        | ((sub8 == 2) & (b_at == 3))
        | ((sub8 == 3) & (a_at == 0))
    )
    there = jnp.where(turned, 3 - place, place)
    cell_a = jnp.where(their == 1, 1, jnp.where(their == 2, 2, 0))
    cell_b = jnp.where(their == 0, 1, jnp.where(their == 3, 2, 3))
    inside = side == 0
    near = [
        jnp.where(inside, 4 * pos + jnp.where(turned, cell_b, cell_a), NOWHERE),
        jnp.where(inside, 4 * pos + jnp.where(turned, cell_a, cell_b), NOWHERE),
    ]
    flip = q & 1
    far = [recv16 + flip, recv16 + 1 - flip]
    send_point = jnp.where(on_edge, 2 * send16 + place, NOWHERE)
    recv_point = jnp.where(on_edge, 2 * recv16 + there, NOWHERE)
    near_point = jnp.where(
        on_edge & inside,
        16 * pos
        + jnp.where((their & 1) == 1, 4 * there, there)
        + jnp.where(their == 1, 3, jnp.where(their == 2, 12, 0)),
        NOWHERE,
    )
    mass = mass_ref[...]
    table = table_ref[...] * mass
    i32 = iota((32, 128), 0)
    i48 = iota((48, 128), 0)
    i128 = iota((128, 128), 0)
    r_on = jnp.zeros((32, 128), F32)
    r_far = jnp.zeros((24, 128), F32)
    sel2 = jnp.zeros((48, 128), F32)
    q_far = jnp.zeros((48, 128), F32)
    q_on = jnp.where(i128 == lane8[0:1], 1.0, 0.0)
    for c in range(4):
        r_on = r_on + jnp.where(i32 == 4 * own16[0:1] + c, table[c : c + 1], 0.0)
    for k in range(4):
        for m in range(2):
            weight = table[4 + 2 * k + m : 5 + 2 * k + m]
            r_on = r_on + jnp.where(i32 == near[m][k : k + 1], weight, 0.0)
            r_far = r_far + jnp.where(i24 == far[m][k : k + 1], weight, 0.0)
        sel2 = sel2 + jnp.where(i48 == send_point[k : k + 1], 1.0, 0.0)
        q_far = q_far + jnp.where(i48 == recv_point[k : k + 1], 1.0, 0.0)
        q_on = q_on + jnp.where(i128 == near_point[k : k + 1], 1.0, 0.0)

    recv4 = recv_row(v4)
    turned4 = (expanded(codes_s, own4) & 1) == 1
    nodes = [-1.0, -1.0 / math.sqrt(5.0), 1.0 / math.sqrt(5.0), 1.0]
    own_add = jnp.zeros((48, 128), F32)
    for k in range(4):
        values = []
        for node in nodes:
            near_edge = [0.5 * linear_weight(m, node) * lagrange(0, -1.0) for m in range(2)]
            values.append(
                jnp.where(
                    cell == CELL_EDGE[k][0],
                    near_edge[0],
                    jnp.where(cell == CELL_EDGE[k][1], near_edge[1], 0.0),
                )
            )
        for t in range(4):
            value = jnp.where(turned4[k : k + 1], values[3 - t], values[t])
            own_add = own_add + jnp.where(i48 == 2 * recv4[k : k + 1] + t, value, 0.0)
    head, rest = halves(own_add)
    group48 = iota((48, 128), 1) >> 5
    own_add = jnp.where(group48 == 1, rest, jnp.where(group48 == 3, 0.0, head)).astype(BF16)

    sel2_16 = sel2.astype(BF16)
    head, rest = halves(r_on)
    r_on3 = jnp.concatenate([head, rest, head, jnp.zeros((32, 128), F32)], axis=0).astype(BF16)
    head, rest = halves(r_far)
    r_far3 = jnp.concatenate([head, rest, head], axis=0).astype(BF16)
    through_on = dot16(sel2_16, r_on3, NT).astype(BF16)
    through = dot16(sel2_16, r_far3, NT)

    def direction(i):
        return jnp.where(i < 8, 0, jnp.where(i < 16, 1, jnp.where(i < 20, 2, 3)))

    there72 = iota((48, 72), 1)
    there72 = jnp.where(there72 < 24, there72, jnp.where(there72 < 48, there72 - 24, there72 - 48))
    same_way = direction(iota((48, 72), 0) >> 1) == direction(there72)
    through = jnp.where(same_way, 0.0, through).astype(BF16)
    masses = jnp.sum(sel2 * mass, axis=1, keepdims=True)
    lane_wide = iota((48, rows), 1)
    base2 = dot16(through_on, pieces_t, NT) + jnp.where(lane_wide == flat, masses, 0.0)
    added = dot16(own_add, pieces_t, NT)
    both = jnp.concatenate([r_on, r_far, jnp.broadcast_to(mass, (8, 128))], axis=0)
    both = dot(both, q_on, NN)
    head, rest = halves(both[0:32])
    near_on = jnp.concatenate([head, rest, head, jnp.zeros((32, 128), F32)], axis=0).astype(BF16)
    head, rest = halves(both[32:56])
    near_far = jnp.concatenate([head, rest, head], axis=0).astype(BF16)
    w_on[...] = dot16(pieces_t, near_on, NN)
    w_on[flat : flat + 1, :] = both[56:57]

    def passive(tile, carry):
        parts = horizontal_parts(tile)
        for r in range(chunks):
            for f in range(3):
                a = st[3 + f, part(r), lanes(tile)].astype(F32)
                bs[f, part(r, 8), :] = horizontal(a, parts)
        for step in range(NSUB):
            for r in range(chunks):
                for f in range(3):
                    a = vertical(bs.at[3 * step + f], r)
                    if f == 0:
                        at = (2 * step + 1) * levels + 8 * r
                        a = a + xs[tile + 2, at : at + 8, :]
                    if step + 1 < NSUB:
                        bs[3 * (step + 1) + f, part(r, 8), :] = horizontal(a, parts)
                    else:
                        state_out[3 + f, part(r), lanes(tile)] = a.astype(BF16)
        for f in range(3):
            state_out[f, :, lanes(tile)] = st[f, :, lanes(tile)]
        return carry

    lax.fori_loop(0, tiles, passive, 0)

    round2 = copies((snd2t, snd2f), (rcv2t, rcv2f), 4)

    def halo_pieces(halo):
        head, rest = halves(halo)
        return jnp.concatenate([head, head, rest], axis=0).astype(BF16)

    round1[3].wait_recv()
    round1[2].wait_recv()
    round1[1].wait_recv()
    halo_f = jnp.concatenate([rcv1f[0], rcv1f[1]], axis=0)
    halo = jnp.concatenate([rcv1t[0], jnp.zeros((8, rows), F32), halo_f], axis=0)
    message = base2[16:32] + dot16(through[16:32], halo_pieces(halo), NN)
    snd2t[1] = message
    round2[1].start()
    round1[0].wait_recv()
    halo = jnp.concatenate([rcv1t[0], rcv1t[1], halo_f], axis=0)
    pieces = halo_pieces(halo)
    message = base2 + dot16(through, pieces, NN)
    snd2f[0] = message[32:40]
    snd2f[1] = message[40:48]
    snd2t[0] = message[0:16]
    round2[2].start()
    round2[3].start()
    round2[0].start()
    near_sum = w_on[...] + dot16(pieces, near_far, TN)
    pick = jnp.concatenate([q_far, q_far], axis=0).astype(BF16)
    for copy in round2:
        copy.wait_recv()
    halo2 = jnp.concatenate([rcv2t[0], rcv2t[1], rcv2f[0], rcv2f[1]], axis=0)
    halo2 = halo2 + halo2[:, flat : flat + 1] * added
    total = near_sum + dot16(jnp.concatenate(halves(halo2), axis=0).astype(BF16), pick, TN)
    inverse = 1.0 / total[flat : flat + 1, :]
    for f in range(fields):
        gll_out[f] = total[f * levels : (f + 1) * levels, :] * inverse
    for copy in round1 + round2:
        copy.wait_send()


def local(
    nf,
    nt,
    crm_state,
    active_levels,
    mix_x,
    drift_speed,
    cond_rate,
    mix_z,
    point_mass,
    neighbor_slots,
    edge_codes,
):
    fields, levels, width = crm_state.shape
    flat = fields * levels
    points = point_mass.shape[0]
    wide = 128 * (flat // 128 + 1)
    tiles = width // 128
    matrix = remap_matrix()
    table = np.zeros((16, points), np.float32)
    table[:12] = np.tile(matrix.T, (1, points // 16))
    vmem = pl.BlockSpec(memory_space=pltpu.VMEM)
    hbm = pl.BlockSpec(memory_space=pltpu.HBM)
    return pl.pallas_call(
        functools.partial(kernel, nf, nt),
        out_shape=(
            jax.ShapeDtypeStruct(crm_state.shape, BF16),
            jax.ShapeDtypeStruct((fields, levels, points), F32),
        ),
        in_specs=[hbm] * 10,
        out_specs=(vmem, vmem),
        scratch_shapes=[
            pltpu.SMEM(neighbor_slots.shape, jnp.int32),
            pltpu.SMEM(edge_codes.shape, jnp.int32),
            pltpu.SMEM(active_levels.shape, jnp.int32),
            pltpu.SMEM(mix_x.shape, F32),
            pltpu.SMEM(drift_speed.shape, F32),
            pltpu.SMEM(cond_rate.shape, F32),
            pltpu.SMEM(mix_z.shape, F32),
            pltpu.VMEM((1, points), F32),
            pltpu.VMEM(table.shape, F32),
            pltpu.VMEM((fields, levels, width), BF16),
            pltpu.VMEM((12, levels + 16, 128), F32),
            pltpu.VMEM((3, levels + 16, 128), F32),
            pltpu.VMEM((width, 128), F32),
            pltpu.VMEM((tiles + 2, 4 * levels, 128), F32),
            pltpu.VMEM((fields, levels + 16, 128), F32),
            pltpu.VMEM((4, levels + 16, 128), F32),
            pltpu.VMEM((wide, 128), F32),
            pltpu.VMEM((wide, 128), F32),
            pltpu.VMEM((2, 8, wide), F32),
            pltpu.VMEM((2, 4, wide), F32),
            pltpu.VMEM((2, 16, wide), F32),
            pltpu.VMEM((2, 8, wide), F32),
            pltpu.VMEM((2, 8, wide), F32),
            pltpu.VMEM((2, 4, wide), F32),
            pltpu.VMEM((2, 16, wide), F32),
            pltpu.VMEM((2, 8, wide), F32),
            pltpu.SemaphoreType.DMA((2,)),
            pltpu.SemaphoreType.DMA((9,)),
            pltpu.SemaphoreType.DMA((8,)),
            pltpu.SemaphoreType.DMA((8,)),
        ],
        compiler_params=pltpu.CompilerParams(collective_id=0, has_side_effects=True, vmem_limit_bytes=40 << 20),
    )(
        *(
            pltpu.with_memory_space_constraint(x, pltpu.HBM)
            for x in (
                neighbor_slots,
                edge_codes,
                active_levels,
                mix_x,
                drift_speed,
                cond_rate,
                mix_z,
                point_mass.reshape(1, points),
                jnp.asarray(table),
                crm_state,
            )
        )
    )


def solution(mesh):
    in_specs = (
        P(None, None, ("face", "tile")),
        P(("face", "tile")),
        P(("face", "tile")),
        P(("face", "tile")),
        P(("face", "tile")),
        P(),
        P(("face", "tile")),
        P(None, ("face", "tile")),
        P(None, ("face", "tile")),
    )
    out_specs = (P(None, None, ("face", "tile")), P(None, None, ("face", "tile")))
    body = functools.partial(local, mesh.shape["face"], mesh.shape["tile"])
    return jax.shard_map(body, mesh=mesh, in_specs=in_specs, out_specs=out_specs, check_vma=False)
```

```python
import functools
import math

import jax
import jax.numpy as jnp
import numpy as np
from jax import lax
from jax.experimental import pallas as pl
from jax.experimental.pallas import tpu as pltpu
from jax.sharding import PartitionSpec as P

NSUB = 2
PER_TIME = 10.0
CELL_EDGE = [[0, 1], [1, 3], [2, 3], [0, 2]]
MESH = pl.DeviceIdType.MESH
F32 = jnp.float32
BF16 = jnp.bfloat16
NOWHERE = -100000
EXP_RATE = 0.3 / math.log(2.0)
NN = (((1,), (0,)), ((), ()))
NT = (((1,), (1,)), ((), ()))
TN = (((0,), (0,)), ((), ()))


def lagrange(q, z):
    centres = [-1.5, -0.5, 0.5, 1.5]
    product = 1.0
    for r in range(4):
        if r != q:
            product = product * (z - centres[r]) / (centres[q] - centres[r])
    return product


def linear_weight(j, z):
    return 0.5 - z if j == 0 else 0.5 + z


def remap_matrix():
    gll_nodes = [-1.0, -1.0 / math.sqrt(5.0), 1.0 / math.sqrt(5.0), 1.0]
    matrix = np.zeros((16, 12))
    for b in range(4):
        for a in range(4):
            p = 4 * b + a
            x = gll_nodes[a]
            y = gll_nodes[b]
            for j in range(2):
                for i in range(2):
                    matrix[p, 2 * j + i] += 0.5 * linear_weight(j, y) * lagrange(
                        1 + i, x
                    ) + 0.5 * linear_weight(i, x) * lagrange(1 + j, y)
            for m in range(2):
                matrix[p, 4 + 6 + m] += 0.5 * linear_weight(m, y) * lagrange(0, x)
                matrix[p, 4 + 2 + m] += 0.5 * linear_weight(m, y) * lagrange(3, x)
                matrix[p, 4 + 0 + m] += 0.5 * linear_weight(m, x) * lagrange(0, y)
                matrix[p, 4 + 4 + m] += 0.5 * linear_weight(m, x) * lagrange(3, y)
    return matrix


def iota(shape, dim):
    return lax.broadcasted_iota(jnp.int32, shape, dim)


def dot(a, b, dims):
    return lax.dot_general(
        a, b, dims, precision=lax.Precision.HIGHEST, preferred_element_type=F32
    )


def dot16(a, b, dims):
    return lax.dot_general(a, b, dims, preferred_element_type=F32)


def halves(x):
    head = x.astype(BF16).astype(F32)
    return head, x - head


def kernel(
    nf,
    nt,
    slots_hbm,
    codes_hbm,
    active_hbm,
    mix_hbm,
    drift_hbm,
    cond_hbm,
    mixz_hbm,
    mass_hbm,
    table_hbm,
    crm_hbm,
    state_out,
    gll_out,
    slots_s,
    codes_s,
    active_s,
    mix_s,
    drift_s,
    cond_s,
    mixz_s,
    mass_ref,
    table_ref,
    st,
    bs,
    cf,
    ones,
    xs,
    zs,
    acc0,
    acc1,
    tend,
    w_on,
    snd1t,
    snd1f,
    snd2t,
    snd2f,
    rcv1t,
    rcv1f,
    rcv2t,
    rcv2f,
    load_sem,
    small_sem,
    send_sem,
    recv_sem,
):
    fields, levels, width = st.shape
    flat = fields * levels
    tiles = width // 128
    rows = tend.shape[0]
    fi = lax.axis_index("face")
    ti = lax.axis_index("tile")
    targets = [
        (fi, lax.rem(ti + nt - 1, nt)),
        (fi, lax.rem(ti + 1, nt)),
        (lax.rem(fi + nf - 1, nf), ti),
        (lax.rem(fi + 1, nf), ti),
    ]
    loads = []
    for p in range(tiles // 2):
        two = slice(256 * p, 256 * (p + 1))
        loads.append(
            pltpu.make_async_copy(crm_hbm.at[:, :, two], st.at[:, :, two], load_sem.at[p])
        )
    loads[0].start()
    smalls = []
    for n, (source, sink) in enumerate(
        (
            (mixz_hbm, mixz_s),
            (mix_hbm, mix_s),
            (drift_hbm, drift_s),
            (cond_hbm, cond_s),
            (active_hbm, active_s),
            (slots_hbm, slots_s),
            (codes_hbm, codes_s),
            (mass_hbm, mass_ref),
            (table_hbm, table_ref),
        )
    ):
        smalls.append(pltpu.make_async_copy(source, sink, small_sem.at[n]))
        smalls[-1].start()
    for copy in loads[1:]:
        copy.start()
    barrier = pltpu.get_barrier_semaphore()
    for target in targets:
        pl.semaphore_signal(barrier, inc=1, device_id=target, device_id_type=MESH)

    lane8 = iota((8, 128), 1)
    sub8 = iota((8, 128), 0)

    own16 = lane8 >> 4
    own4 = (lane8 & 31) >> 2

    def expanded(source, own):
        key = sub8 * 32 + own
        out = jnp.full((8, 128), -1, jnp.int32)
        for k in range(4):
            for e in range(8):
                out = jnp.where(key == k * 32 + e, source[k, e], out)
        return out

    def base_of(side):
        return jnp.where(
            side == 1,
            0,
            jnp.where(side == 2, 8, jnp.where(side == 3, 16, jnp.where(side == 4, 20, NOWHERE))),
        )

    def send_row(v, own):
        side = v >> 3
        rank = jnp.zeros((8, 128), jnp.int32)
        for k in range(4):
            for e in range(8):
                rank = rank + jnp.where((side == (slots_s[k, e] >> 3)) & (own > e), 2, 0)
        return base_of(side) + rank

    def recv_row(v):
        side = v >> 3
        rank = jnp.zeros((8, 128), jnp.int32)
        for k in range(4):
            for e in range(8):
                other = slots_s[k, e]
                rank = rank + jnp.where((side == (other >> 3)) & (v > other), 2, 0)
        return base_of(side) + rank

    lane_r = iota((256, 128), 0) >> 5
    lane_n = iota((256, 128), 1) & 31
    for p in range(width // 256):
        ones[256 * p : 256 * (p + 1), :] = jnp.where(lane_n == lane_r + 8 * p, 1.0, 0.0)
    acc0[...] = jnp.zeros_like(acc0)
    acc1[...] = jnp.zeros_like(acc1)
    tend[flat:rows, :] = jnp.zeros((rows - flat, 128), F32)
    blank = jnp.zeros((8, 128), F32)
    for n in range(bs.shape[0]):
        bs[n, 0:8, :] = blank
        bs[n, levels + 8 : levels + 16, :] = blank
    for n in range(cf.shape[0]):
        cf[n, 0:8, :] = blank
        cf[n, levels + 8 : levels + 16, :] = blank

    for copy in smalls:
        copy.wait()

    chunks = levels // 8
    for r in range(chunks):
        upper, lower = blank, blank
        for s in range(8):
            l = 8 * r + s
            if l < levels - 1:
                upper = jnp.where(sub8 == s, mixz_s[l], upper)
            if l > 0:
                lower = jnp.where(sub8 == s, mixz_s[l - 1], lower)
        cf[0, 8 * r + 8 : 8 * r + 16, :] = upper
        cf[1, 8 * r + 8 : 8 * r + 16, :] = lower
        cf[2, 8 * r + 8 : 8 * r + 16, :] = 1.0 - upper - lower

    v4 = expanded(slots_s, own4)
    row4 = jnp.where((lane8 & 32) == 0, send_row(v4, own4), NOWHERE)
    cell = lane8[0:1] & 3
    i24 = iota((24, 128), 0)
    sel1 = jnp.zeros((24, 128), F32)
    for k in range(4):
        first = row4[k : k + 1]
        goal = jnp.where(
            cell == CELL_EDGE[k][0],
            first,
            jnp.where(cell == CELL_EDGE[k][1], first + 1, NOWHERE),
        )
        sel1 = sel1 + jnp.where(i24 == goal, 1.0, 0.0)

    def part(r, shift=0):
        return slice(8 * r + shift, 8 * r + 8 + shift)

    def vertical(buffer, r):
        return (
            cf[2, part(r, 8), :] * buffer[part(r, 8), :]
            + cf[0, part(r, 8), :] * buffer[part(r, 9), :]
            + cf[1, part(r, 8), :] * buffer[part(r, 7), :]
        )

    east_at = (lane8 & 96) | ((lane8 + 1) & 31)
    west_at = (lane8 & 96) | ((lane8 + 31) & 31)
    group = lane8 >> 5

    def per_column(source, tile):
        out = jnp.full((8, 128), source[4 * tile])
        for g in range(1, 4):
            out = jnp.where(group == g, source[4 * tile + g], out)
        return out

    def horizontal_parts(tile):
        mix = per_column(mix_s, tile)
        half = 0.5 * per_column(drift_s, tile)
        return 1.0 - 2.0 * mix, mix - half, mix + half

    def horizontal(a, parts):
        mid, east, west = parts
        return (
            a * mid
            + east * jnp.take_along_axis(a, east_at, axis=1)
            + west * jnp.take_along_axis(a, west_at, axis=1)
        )

    def lanes(tile):
        return pl.ds(pl.multiple_of(tile * 128, 128), 128)

    def gather_sums(slot, tile):
        head, rest = halves(xs[slot])
        pick = ones[128 * tile : 128 * (tile + 1), :]
        sums = dot16(
            jnp.concatenate([head, rest], axis=1), jnp.concatenate([pick, pick], axis=0), NN
        )
        for n in range(2):
            acc1[n] += sums[n * levels : (n + 1) * levels]

    def active_tile(tile, slot, lot):
        parts = horizontal_parts(tile)
        limit = per_column(active_s, tile)
        rate = per_column(cond_s, tile)
        at_lanes = slice(128 * tile, 128 * (tile + 1))
        for r in range(chunks):
            for f in range(3):
                a = st[f, part(r), at_lanes].astype(F32)
                bs[lot + f, part(r, 8), :] = horizontal(a, parts)
        for step in range(NSUB):
            for r in range(chunks):
                t, qv, ql = (vertical(bs.at[lot + 3 * step + f], r) for f in range(3))
                alive = sub8 + 8 * r < limit
                sat = jnp.exp2(EXP_RATE * t - 1.0)
                cond = jnp.where(alive, jnp.maximum(rate * (qv - sat), -ql), 0.0)
                qv = qv - cond
                ql = ql + cond
                t = t + 0.5 * cond
                freeze = jnp.where(alive, 0.15 * ql * (1.0 - jnp.tanh(t)), 0.0)
                ql = ql - freeze
                t = t + 0.1 * freeze
                zs[tile, step, part(r), :] = freeze
                if step + 1 < NSUB:
                    for f, a in enumerate((t, qv, ql)):
                        bs[lot + 3 * (step + 1) + f, part(r, 8), :] = horizontal(a, parts)
                else:
                    xs[slot, 8 * r : 8 * r + 8, :] = qv
                    xs[slot, levels + 8 * r : levels + 8 * r + 8, :] = ql
                    for f, a in enumerate((t, qv, ql)):
                        st[f, part(r), at_lanes] = a.astype(BF16)

    for p in range(tiles // 2):
        loads[p].wait()
        start = jnp.concatenate(
            [st[f, :, 256 * p : 256 * (p + 1)].astype(F32) for f in range(fields)], axis=0
        )
        sums = dot16(start, ones[256 * p : 256 * (p + 1), :], NN)
        for f in range(fields):
            acc0[f, 8 : levels + 8, :] += sums[f * levels : (f + 1) * levels]
        for tile in (2 * p, 2 * p + 1):
            if tile >= 2:
                gather_sums(tile - 2, tile - 2)
            active_tile(tile, tile, 6 * (tile % 2))
    gather_sums(tiles - 2, tiles - 2)
    gather_sums(tiles - 1, tiles - 1)

    scale = PER_TIME / 32.0
    for r in range(chunks):
        upper, lower, middle = (cf[n, part(r, 8), :] for n in range(3))
        two_up = scale * upper * cf[0, part(r, 9), :]
        one_up = scale * upper * (middle + cf[2, part(r, 9), :])
        one_down = scale * lower * (middle + cf[2, part(r, 7), :])
        two_down = scale * lower * cf[1, part(r, 7), :]
        same = scale * (upper * upper + lower * lower + middle * middle - 1.0)
        mixed = []
        for f in range(fields):
            mixed.append(
                same * acc0[f, part(r, 8), :]
                + (one_up * acc0[f, part(r, 9), :] + one_down * acc0[f, part(r, 7), :])
                + (two_up * acc0[f, part(r, 10), :] + two_down * acc0[f, part(r, 6), :])
            )
        vapour = scale * (acc1[0, part(r), :] - acc0[1, part(r, 8), :])
        liquid = scale * (acc1[1, part(r), :] - acc0[2, part(r, 8), :])
        cond_sum = mixed[1] - vapour
        freeze_sum = mixed[2] + cond_sum - liquid
        mixed[0] = mixed[0] + 0.5 * cond_sum + 0.1 * freeze_sum
        mixed[1] = vapour
        mixed[2] = liquid
        mixed[3] = mixed[3] + freeze_sum
        for f in range(fields):
            at = f * levels + 8 * r
            tend[at : at + 8, :] = mixed[f]

    head, rest = halves(tend[...])
    wide_group = iota((rows, 128), 1) >> 5
    pieces_t = jnp.where(wide_group < 2, head, jnp.where(wide_group == 2, rest, 0.0)).astype(BF16)
    message = dot16(sel1.astype(BF16), pieces_t, NT)
    snd1t[0] = message[0:8]
    snd1t[1] = message[8:16]
    snd1f[0] = message[16:20]
    snd1f[1] = message[20:24]

    pl.semaphore_wait(barrier, 4)

    def copies(sends, recvs, base):
        out = []
        for o, target in enumerate(targets):
            source, sink = (sends[0], recvs[0]) if o < 2 else (sends[1], recvs[1])
            out.append(
                pltpu.make_async_remote_copy(
                    src_ref=source.at[o % 2],
                    dst_ref=sink.at[1 - o % 2],
                    send_sem=send_sem.at[base + o],
                    recv_sem=recv_sem.at[base + (o ^ 1)],
                    device_id=target,
                    device_id_type=MESH,
                )
            )
        return out

    round1 = copies((snd1t, snd1f), (rcv1t, rcv1f), 0)
    for copy in round1:
        copy.start()

    v = expanded(slots_s, own16)
    q = expanded(codes_s, own16)
    side, pos = v >> 3, v & 7
    their, turned = q >> 1, (q & 1) == 1
    send16, recv16 = send_row(v, own16), recv_row(v)
    point = lane8 & 15
    a_at, b_at = point & 3, point >> 2
    place = jnp.where((sub8 & 1) == 0, a_at, b_at)
    on_edge = (
        ((sub8 == 0) & (b_at == 0))
        | ((sub8 == 1) & (a_at == 3))
        | ((sub8 == 2) & (b_at == 3))
        | ((sub8 == 3) & (a_at == 0))
    )
    there = jnp.where(turned, 3 - place, place)
    cell_a = jnp.where(their == 1, 1, jnp.where(their == 2, 2, 0))
    cell_b = jnp.where(their == 0, 1, jnp.where(their == 3, 2, 3))
    inside = side == 0
    near = [
        jnp.where(inside, 4 * pos + jnp.where(turned, cell_b, cell_a), NOWHERE),
        jnp.where(inside, 4 * pos + jnp.where(turned, cell_a, cell_b), NOWHERE),
    ]
    flip = q & 1
    far = [recv16 + flip, recv16 + 1 - flip]
    send_point = jnp.where(on_edge, 2 * send16 + place, NOWHERE)
    recv_point = jnp.where(on_edge, 2 * recv16 + there, NOWHERE)
    near_point = jnp.where(
        on_edge & inside,
        16 * pos
        + jnp.where((their & 1) == 1, 4 * there, there)
        + jnp.where(their == 1, 3, jnp.where(their == 2, 12, 0)),
        NOWHERE,
    )
    mass = mass_ref[...]
    table = table_ref[...] * mass
    i32 = iota((32, 128), 0)
    i48 = iota((48, 128), 0)
    i128 = iota((128, 128), 0)
    r_on = jnp.zeros((32, 128), F32)
    r_far = jnp.zeros((24, 128), F32)
    sel2 = jnp.zeros((48, 128), F32)
    q_far = jnp.zeros((48, 128), F32)
    q_on = jnp.where(i128 == lane8[0:1], 1.0, 0.0)
    for c in range(4):
        r_on = r_on + jnp.where(i32 == 4 * own16[0:1] + c, table[c : c + 1], 0.0)
    for k in range(4):
        for m in range(2):
            weight = table[4 + 2 * k + m : 5 + 2 * k + m]
            r_on = r_on + jnp.where(i32 == near[m][k : k + 1], weight, 0.0)
            r_far = r_far + jnp.where(i24 == far[m][k : k + 1], weight, 0.0)
        sel2 = sel2 + jnp.where(i48 == send_point[k : k + 1], 1.0, 0.0)
        q_far = q_far + jnp.where(i48 == recv_point[k : k + 1], 1.0, 0.0)
        q_on = q_on + jnp.where(i128 == near_point[k : k + 1], 1.0, 0.0)

    recv4 = recv_row(v4)
    turned4 = (expanded(codes_s, own4) & 1) == 1
    nodes = [-1.0, -1.0 / math.sqrt(5.0), 1.0 / math.sqrt(5.0), 1.0]
    own_add = jnp.zeros((48, 128), F32)
    for k in range(4):
        values = []
        for node in nodes:
            near_edge = [0.5 * linear_weight(m, node) * lagrange(0, -1.0) for m in range(2)]
            values.append(
                jnp.where(
                    cell == CELL_EDGE[k][0],
                    near_edge[0],
                    jnp.where(cell == CELL_EDGE[k][1], near_edge[1], 0.0),
                )
            )
        for t in range(4):
            value = jnp.where(turned4[k : k + 1], values[3 - t], values[t])
            own_add = own_add + jnp.where(i48 == 2 * recv4[k : k + 1] + t, value, 0.0)
    head, rest = halves(own_add)
    group48 = iota((48, 128), 1) >> 5
    own_add = jnp.where(group48 == 1, rest, jnp.where(group48 == 3, 0.0, head)).astype(BF16)

    sel2_16 = sel2.astype(BF16)
    head, rest = halves(r_on)
    r_on3 = jnp.concatenate([head, rest, head, jnp.zeros((32, 128), F32)], axis=0).astype(BF16)
    head, rest = halves(r_far)
    r_far3 = jnp.concatenate([head, rest, head], axis=0).astype(BF16)
    through_on = dot16(sel2_16, r_on3, NT).astype(BF16)
    through = dot16(sel2_16, r_far3, NT)

    def direction(i):
        return jnp.where(i < 8, 0, jnp.where(i < 16, 1, jnp.where(i < 20, 2, 3)))

    there72 = iota((48, 72), 1)
    there72 = jnp.where(there72 < 24, there72, jnp.where(there72 < 48, there72 - 24, there72 - 48))
    same_way = direction(iota((48, 72), 0) >> 1) == direction(there72)
    through = jnp.where(same_way, 0.0, through).astype(BF16)
    masses = jnp.sum(sel2 * mass, axis=1, keepdims=True)
    lane_wide = iota((48, rows), 1)
    base2 = dot16(through_on, pieces_t, NT) + jnp.where(lane_wide == flat, masses, 0.0)
    added = dot16(own_add, pieces_t, NT)
    both = jnp.concatenate([r_on, r_far, jnp.broadcast_to(mass, (8, 128))], axis=0)
    both = dot(both, q_on, NN)
    head, rest = halves(both[0:32])
    near_on = jnp.concatenate([head, rest, head, jnp.zeros((32, 128), F32)], axis=0).astype(BF16)
    head, rest = halves(both[32:56])
    near_far = jnp.concatenate([head, rest, head], axis=0).astype(BF16)
    w_on[...] = dot16(pieces_t, near_on, NN)
    w_on[flat : flat + 1, :] = both[56:57]

    def passive(tile, carry):
        parts = horizontal_parts(tile)
        for r in range(chunks):
            for f in range(3):
                a = st[3 + f, part(r), lanes(tile)].astype(F32)
                bs[f, part(r, 8), :] = horizontal(a, parts)
        for step in range(NSUB):
            for r in range(chunks):
                for f in range(3):
                    a = vertical(bs.at[3 * step + f], r)
                    if f == 0:
                        a = a + zs[tile, step, part(r), :]
                    if step + 1 < NSUB:
                        bs[3 * (step + 1) + f, part(r, 8), :] = horizontal(a, parts)
                    else:
                        state_out[3 + f, part(r), lanes(tile)] = a.astype(BF16)
        for f in range(3):
            state_out[f, :, lanes(tile)] = st[f, :, lanes(tile)]
        return carry

    lax.fori_loop(0, tiles, passive, 0)

    round2 = copies((snd2t, snd2f), (rcv2t, rcv2f), 4)

    def halo_pieces(halo):
        head, rest = halves(halo)
        return jnp.concatenate([head, head, rest], axis=0).astype(BF16)

    round1[3].wait_recv()
    round1[2].wait_recv()
    round1[1].wait_recv()
    halo_f = jnp.concatenate([rcv1f[0], rcv1f[1]], axis=0)
    halo = jnp.concatenate([rcv1t[0], jnp.zeros((8, rows), F32), halo_f], axis=0)
    message = base2[16:32] + dot16(through[16:32], halo_pieces(halo), NN)
    snd2t[1] = message
    round2[1].start()
    round1[0].wait_recv()
    halo = jnp.concatenate([rcv1t[0], rcv1t[1], halo_f], axis=0)
    pieces = halo_pieces(halo)
    message = base2 + dot16(through, pieces, NN)
    snd2f[0] = message[32:40]
    snd2f[1] = message[40:48]
    snd2t[0] = message[0:16]
    round2[2].start()
    round2[3].start()
    round2[0].start()
    near_sum = w_on[...] + dot16(pieces, near_far, TN)
    pick = jnp.concatenate([q_far, q_far], axis=0).astype(BF16)
    for copy in round2:
        copy.wait_recv()
    halo2 = jnp.concatenate([rcv2t[0], rcv2t[1], rcv2f[0], rcv2f[1]], axis=0)
    halo2 = halo2 + halo2[:, flat : flat + 1] * added
    total = near_sum + dot16(jnp.concatenate(halves(halo2), axis=0).astype(BF16), pick, TN)
    inverse = 1.0 / total[flat : flat + 1, :]
    for f in range(fields):
        gll_out[f] = total[f * levels : (f + 1) * levels, :] * inverse
    for copy in round1 + round2:
        copy.wait_send()


def local(
    nf,
    nt,
    crm_state,
    active_levels,
    mix_x,
    drift_speed,
    cond_rate,
    mix_z,
    point_mass,
    neighbor_slots,
    edge_codes,
):
    fields, levels, width = crm_state.shape
    flat = fields * levels
    points = point_mass.shape[0]
    wide = 128 * (flat // 128 + 1)
    tiles = width // 128
    matrix = remap_matrix()
    table = np.zeros((16, points), np.float32)
    table[:12] = np.tile(matrix.T, (1, points // 16))
    vmem = pl.BlockSpec(memory_space=pltpu.VMEM)
    hbm = pl.BlockSpec(memory_space=pltpu.HBM)
    state, gll = pl.pallas_call(
        functools.partial(kernel, nf, nt),
        out_shape=(
            jax.ShapeDtypeStruct(crm_state.shape, BF16),
            jax.ShapeDtypeStruct((fields, levels, points), F32),
        ),
        in_specs=[hbm] * 10,
        out_specs=(vmem, vmem),
        scratch_shapes=[
            pltpu.SMEM(neighbor_slots.shape, jnp.int32),
            pltpu.SMEM(edge_codes.shape, jnp.int32),
            pltpu.SMEM(active_levels.shape, jnp.int32),
            pltpu.SMEM(mix_x.shape, F32),
            pltpu.SMEM(drift_speed.shape, F32),
            pltpu.SMEM(cond_rate.shape, F32),
            pltpu.SMEM(mix_z.shape, F32),
            pltpu.VMEM((1, points), F32),
            pltpu.VMEM(table.shape, F32),
            pltpu.VMEM((fields, levels, width), BF16),
            pltpu.VMEM((12, levels + 16, 128), F32),
            pltpu.VMEM((3, levels + 16, 128), F32),
            pltpu.VMEM((width, 128), F32),
            pltpu.VMEM((tiles, 2 * levels, 128), F32),
            pltpu.VMEM((tiles, NSUB, levels, 128), F32),
            pltpu.VMEM((fields, levels + 16, 128), F32),
            pltpu.VMEM((2, levels, 128), F32),
            pltpu.VMEM((wide, 128), F32),
            pltpu.VMEM((wide, 128), F32),
            pltpu.VMEM((2, 8, wide), F32),
            pltpu.VMEM((2, 4, wide), F32),
            pltpu.VMEM((2, 16, wide), F32),
            pltpu.VMEM((2, 8, wide), F32),
            pltpu.VMEM((2, 8, wide), F32),
            pltpu.VMEM((2, 4, wide), F32),
            pltpu.VMEM((2, 16, wide), F32),
            pltpu.VMEM((2, 8, wide), F32),
            pltpu.SemaphoreType.DMA((tiles // 2,)),
            pltpu.SemaphoreType.DMA((9,)),
            pltpu.SemaphoreType.DMA((8,)),
            pltpu.SemaphoreType.DMA((8,)),
        ],
        compiler_params=pltpu.CompilerParams(collective_id=0, has_side_effects=True, vmem_limit_bytes=40 << 20),
    )(
        *(
            pltpu.with_memory_space_constraint(x, pltpu.HBM)
            for x in (
                neighbor_slots,
                edge_codes,
                active_levels,
                mix_x,
                drift_speed,
                cond_rate,
                mix_z,
                point_mass.reshape(1, points),
                jnp.asarray(table),
                crm_state,
            )
        )
    )
    return pl.pallas_call(
        write_out,
        out_shape=(
            jax.ShapeDtypeStruct(state.shape, BF16),
            jax.ShapeDtypeStruct(gll.shape, F32),
        ),
        in_specs=[vmem, vmem],
        out_specs=(hbm, hbm),
        scratch_shapes=[pltpu.SemaphoreType.DMA((2,))],
        compiler_params=pltpu.CompilerParams(vmem_limit_bytes=1 << 20),
    )(state, gll)


def write_out(state, gll, state_out, gll_out, sem):
    first = pltpu.make_async_copy(state, state_out, sem.at[0])
    second = pltpu.make_async_copy(gll, gll_out, sem.at[1])
    first.start()
    second.start()
    first.wait()
    second.wait()


def solution(mesh):
    in_specs = (
        P(None, None, ("face", "tile")),
        P(("face", "tile")),
        P(("face", "tile")),
        P(("face", "tile")),
        P(("face", "tile")),
        P(),
        P(("face", "tile")),
        P(None, ("face", "tile")),
        P(None, ("face", "tile")),
    )
    out_specs = (P(None, None, ("face", "tile")), P(None, None, ("face", "tile")))
    body = functools.partial(local, mesh.shape["face"], mesh.shape["tile"])
    return jax.shard_map(body, mesh=mesh, in_specs=in_specs, out_specs=out_specs, check_vma=False)
```

```python
import functools
import math

import jax
import jax.numpy as jnp
import numpy as np
from jax import lax
from jax.experimental import pallas as pl
from jax.experimental.pallas import tpu as pltpu
from jax.sharding import PartitionSpec as P

NSUB = 2
PER_TIME = 10.0
CELL_EDGE = [[0, 1], [1, 3], [2, 3], [0, 2]]
MESH = pl.DeviceIdType.MESH
F32 = jnp.float32
BF16 = jnp.bfloat16
NOWHERE = -100000
LEAST_ACTIVE = 18
EXP_RATE = 0.3 / math.log(2.0)
NN = (((1,), (0,)), ((), ()))
NT = (((1,), (1,)), ((), ()))
TN = (((0,), (0,)), ((), ()))


def lagrange(q, z):
    centres = [-1.5, -0.5, 0.5, 1.5]
    product = 1.0
    for r in range(4):
        if r != q:
            product = product * (z - centres[r]) / (centres[q] - centres[r])
    return product


def linear_weight(j, z):
    return 0.5 - z if j == 0 else 0.5 + z


def remap_matrix():
    gll_nodes = [-1.0, -1.0 / math.sqrt(5.0), 1.0 / math.sqrt(5.0), 1.0]
    matrix = np.zeros((16, 12))
    for b in range(4):
        for a in range(4):
            p = 4 * b + a
            x = gll_nodes[a]
            y = gll_nodes[b]
            for j in range(2):
                for i in range(2):
                    matrix[p, 2 * j + i] += 0.5 * linear_weight(j, y) * lagrange(
                        1 + i, x
                    ) + 0.5 * linear_weight(i, x) * lagrange(1 + j, y)
            for m in range(2):
                matrix[p, 4 + 6 + m] += 0.5 * linear_weight(m, y) * lagrange(0, x)
                matrix[p, 4 + 2 + m] += 0.5 * linear_weight(m, y) * lagrange(3, x)
                matrix[p, 4 + 0 + m] += 0.5 * linear_weight(m, x) * lagrange(0, y)
                matrix[p, 4 + 4 + m] += 0.5 * linear_weight(m, x) * lagrange(3, y)
    return matrix


def iota(shape, dim):
    return lax.broadcasted_iota(jnp.int32, shape, dim)


def dot(a, b, dims):
    return lax.dot_general(
        a, b, dims, precision=lax.Precision.HIGHEST, preferred_element_type=F32
    )


def dot16(a, b, dims):
    return lax.dot_general(a, b, dims, preferred_element_type=F32)


def halves(x):
    head = x.astype(BF16).astype(F32)
    return head, x - head


def kernel(
    nf,
    nt,
    slots_hbm,
    codes_hbm,
    active_hbm,
    mix_hbm,
    drift_hbm,
    cond_hbm,
    mixz_hbm,
    mass_hbm,
    table_hbm,
    crm_hbm,
    state_out,
    gll_out,
    slots_s,
    codes_s,
    active_s,
    mix_s,
    drift_s,
    cond_s,
    mixz_s,
    mass_ref,
    table_ref,
    st,
    bs,
    fs,
    cf,
    ones,
    xs,
    zs,
    acc0,
    acc1,
    tend,
    w_on,
    snd1t,
    snd1f,
    snd2t,
    snd2f,
    rcv1t,
    rcv1f,
    rcv2t,
    rcv2f,
    load_sem,
    small_sem,
    send_sem,
    recv_sem,
):
    fields, levels, width = st.shape
    flat = fields * levels
    tiles = width // 128
    rows = tend.shape[0]
    fi = lax.axis_index("face")
    ti = lax.axis_index("tile")
    targets = [
        (fi, lax.rem(ti + nt - 1, nt)),
        (fi, lax.rem(ti + 1, nt)),
        (lax.rem(fi + nf - 1, nf), ti),
        (lax.rem(fi + 1, nf), ti),
    ]
    loads = []
    for p in range(tiles // 2):
        two = slice(256 * p, 256 * (p + 1))
        loads.append(
            pltpu.make_async_copy(crm_hbm.at[:, :, two], st.at[:, :, two], load_sem.at[p])
        )
    loads[0].start()
    smalls = []
    for n, (source, sink) in enumerate(
        (
            (mixz_hbm, mixz_s),
            (mix_hbm, mix_s),
            (drift_hbm, drift_s),
            (cond_hbm, cond_s),
            (active_hbm, active_s),
            (slots_hbm, slots_s),
            (codes_hbm, codes_s),
            (mass_hbm, mass_ref),
            (table_hbm, table_ref),
        )
    ):
        smalls.append(pltpu.make_async_copy(source, sink, small_sem.at[n]))
        smalls[-1].start()
    for copy in loads[1:]:
        copy.start()
    barrier = pltpu.get_barrier_semaphore()
    for target in targets:
        pl.semaphore_signal(barrier, inc=1, device_id=target, device_id_type=MESH)

    lane8 = iota((8, 128), 1)
    sub8 = iota((8, 128), 0)

    own16 = lane8 >> 4
    own4 = (lane8 & 31) >> 2

    def expanded(source, own):
        key = sub8 * 32 + own
        out = jnp.full((8, 128), -1, jnp.int32)
        for k in range(4):
            for e in range(8):
                out = jnp.where(key == k * 32 + e, source[k, e], out)
        return out

    def base_of(side):
        return jnp.where(
            side == 1,
            0,
            jnp.where(side == 2, 8, jnp.where(side == 3, 16, jnp.where(side == 4, 20, NOWHERE))),
        )

    def send_row(v, own):
        side = v >> 3
        rank = jnp.zeros((8, 128), jnp.int32)
        for k in range(4):
            for e in range(8):
                rank = rank + jnp.where((side == (slots_s[k, e] >> 3)) & (own > e), 2, 0)
        return base_of(side) + rank

    def recv_row(v):
        side = v >> 3
        rank = jnp.zeros((8, 128), jnp.int32)
        for k in range(4):
            for e in range(8):
                other = slots_s[k, e]
                rank = rank + jnp.where((side == (other >> 3)) & (v > other), 2, 0)
        return base_of(side) + rank

    lane_r = iota((256, 128), 0) >> 5
    lane_n = iota((256, 128), 1) & 31
    for p in range(width // 256):
        ones[256 * p : 256 * (p + 1), :] = jnp.where(lane_n == lane_r + 8 * p, 1.0, 0.0)
    acc0[...] = jnp.zeros_like(acc0)
    acc1[...] = jnp.zeros_like(acc1)
    tend[flat:rows, :] = jnp.zeros((rows - flat, 128), F32)
    blank = jnp.zeros((8, 128), F32)
    for n in range(bs.shape[0]):
        bs[n, 0:8, :] = blank
        bs[n, levels + 8 : levels + 16, :] = blank
        fs[n, 0:8, :] = blank
    for n in range(cf.shape[0]):
        cf[n, 0:8, :] = blank
        cf[n, levels + 8 : levels + 16, :] = blank

    for copy in smalls:
        copy.wait()

    chunks = levels // 8
    for r in range(chunks):
        upper, lower = blank, blank
        for s in range(8):
            l = 8 * r + s
            if l < levels - 1:
                upper = jnp.where(sub8 == s, mixz_s[l], upper)
            if l > 0:
                lower = jnp.where(sub8 == s, mixz_s[l - 1], lower)
        cf[0, 8 * r + 8 : 8 * r + 16, :] = upper
        cf[1, 8 * r + 8 : 8 * r + 16, :] = lower
        cf[2, 8 * r + 8 : 8 * r + 16, :] = 1.0 - upper - lower

    def part(r, shift=0):
        return slice(8 * r + shift, 8 * r + 8 + shift)

    def vertical(n, r):
        b = bs[n, part(r, 8), :]
        flux = cf[0, part(r, 8), :] * (bs[n, part(r, 9), :] - b)
        fs[n, part(r, 8), :] = flux
        return b + flux - fs[n, part(r, 7), :]

    east_at = (lane8 & 96) | ((lane8 + 1) & 31)
    west_at = (lane8 & 96) | ((lane8 + 31) & 31)
    group = lane8 >> 5

    def per_column(source, tile):
        out = jnp.full((8, 128), source[4 * tile])
        for g in range(1, 4):
            out = jnp.where(group == g, source[4 * tile + g], out)
        return out

    def horizontal_parts(tile):
        mix = per_column(mix_s, tile)
        half = 0.5 * per_column(drift_s, tile)
        return 1.0 - 2.0 * mix, mix - half, mix + half

    def horizontal(a, parts):
        mid, east, west = parts
        return (
            a * mid
            + east * jnp.take_along_axis(a, east_at, axis=1)
            + west * jnp.take_along_axis(a, west_at, axis=1)
        )

    def lanes(tile):
        return pl.ds(pl.multiple_of(tile * 128, 128), 128)

    def gather_sums(slot, tile):
        head, rest = halves(xs[slot])
        pick = ones[128 * tile : 128 * (tile + 1), :]
        sums = dot16(
            jnp.concatenate([head, rest], axis=1), jnp.concatenate([pick, pick], axis=0), NN
        )
        for n in range(2):
            acc1[n] += sums[n * levels : (n + 1) * levels]

    def active_tile(tile, slot, lot, chunk):
        parts = horizontal_parts(tile)
        limit = per_column(active_s, tile)
        rate = per_column(cond_s, tile)
        at_lanes = slice(128 * tile, 128 * (tile + 1))
        for r in range(chunks):
            for f in range(3):
                bs[lot + f, part(r, 8), :] = horizontal(chunk[f][r], parts)
        for step in range(NSUB):
            for r in range(chunks):
                t, qv, ql = (vertical(lot + 3 * step + f, r) for f in range(3))
                always = 8 * r + 8 <= LEAST_ACTIVE
                alive = sub8 + 8 * r < limit
                sat = jnp.exp2(EXP_RATE * t - 1.0)
                cond = jnp.maximum(rate * (qv - sat), -ql)
                if not always:
                    cond = jnp.where(alive, cond, 0.0)
                qv = qv - cond
                ql = ql + cond
                t = t + 0.5 * cond
                freeze = 0.15 * ql * (1.0 - jnp.tanh(t))
                if not always:
                    freeze = jnp.where(alive, freeze, 0.0)
                ql = ql - freeze
                t = t + 0.1 * freeze
                zs[tile, step, part(r), :] = freeze
                if step + 1 < NSUB:
                    for f, a in enumerate((t, qv, ql)):
                        bs[lot + 3 * (step + 1) + f, part(r, 8), :] = horizontal(a, parts)
                else:
                    xs[slot, 8 * r : 8 * r + 8, :] = qv
                    xs[slot, levels + 8 * r : levels + 8 * r + 8, :] = ql
                    for f, a in enumerate((t, qv, ql)):
                        st[f, part(r), at_lanes] = a.astype(BF16)

    for p in range(tiles // 2):
        if p < 2:
            for copy in loads[p : (1, tiles // 2)[p]]:
                copy.wait()
        if p == 0:
            v4 = expanded(slots_s, own4)
            row4 = jnp.where((lane8 & 32) == 0, send_row(v4, own4), NOWHERE)
            cell = lane8[0:1] & 3
            i24 = iota((24, 128), 0)
            sel1 = jnp.zeros((24, 128), F32)
            for k in range(4):
                first = row4[k : k + 1]
                goal = jnp.where(
                    cell == CELL_EDGE[k][0],
                    first,
                    jnp.where(cell == CELL_EDGE[k][1], first + 1, NOWHERE),
                )
                sel1 = sel1 + jnp.where(i24 == goal, 1.0, 0.0)

        chunk = [
            [
                [
                    st[f, part(r), 128 * tile : 128 * (tile + 1)].astype(F32)
                    for r in range(chunks)
                ]
                for f in range(fields)
            ]
            for tile in (2 * p, 2 * p + 1)
        ]
        start = jnp.concatenate(
            [
                jnp.concatenate([chunk[0][f][r], chunk[1][f][r]], axis=1)
                for f in range(fields)
                for r in range(chunks)
            ],
            axis=0,
        )
        sums = dot16(start, ones[256 * p : 256 * (p + 1), :], NN)
        for f in range(fields):
            acc0[f, 8 : levels + 8, :] += sums[f * levels : (f + 1) * levels]
        for tile in (2 * p, 2 * p + 1):
            if tile >= 2:
                gather_sums(tile - 2, tile - 2)
            active_tile(tile, tile, 6 * (tile % 2), chunk[tile % 2])
    gather_sums(tiles - 2, tiles - 2)
    gather_sums(tiles - 1, tiles - 1)

    scale = PER_TIME / 32.0
    for r in range(chunks):
        upper, lower, middle = (cf[n, part(r, 8), :] for n in range(3))
        two_up = scale * upper * cf[0, part(r, 9), :]
        one_up = scale * upper * (middle + cf[2, part(r, 9), :])
        one_down = scale * lower * (middle + cf[2, part(r, 7), :])
        two_down = scale * lower * cf[1, part(r, 7), :]
        same = scale * (upper * upper + lower * lower + middle * middle - 1.0)
        mixed = []
        for f in range(fields):
            mixed.append(
                same * acc0[f, part(r, 8), :]
                + (one_up * acc0[f, part(r, 9), :] + one_down * acc0[f, part(r, 7), :])
                + (two_up * acc0[f, part(r, 10), :] + two_down * acc0[f, part(r, 6), :])
            )
        vapour = scale * (acc1[0, part(r), :] - acc0[1, part(r, 8), :])
        liquid = scale * (acc1[1, part(r), :] - acc0[2, part(r, 8), :])
        cond_sum = mixed[1] - vapour
        freeze_sum = mixed[2] + cond_sum - liquid
        mixed[0] = mixed[0] + 0.5 * cond_sum + 0.1 * freeze_sum
        mixed[1] = vapour
        mixed[2] = liquid
        mixed[3] = mixed[3] + freeze_sum
        for f in range(fields):
            at = f * levels + 8 * r
            tend[at : at + 8, :] = mixed[f]

    head, rest = halves(tend[...])
    wide_group = iota((rows, 128), 1) >> 5
    pieces_t = jnp.where(wide_group < 2, head, rest).astype(BF16)
    message = dot16(sel1.astype(BF16), pieces_t, NT)
    snd1t[0] = message[0:8]
    snd1t[1] = message[8:16]
    snd1f[0] = message[16:20]
    snd1f[1] = message[20:24]

    pl.semaphore_wait(barrier, 4)

    def copies(sends, recvs, base):
        out = []
        for o, target in enumerate(targets):
            source, sink = (sends[0], recvs[0]) if o < 2 else (sends[1], recvs[1])
            out.append(
                pltpu.make_async_remote_copy(
                    src_ref=source.at[o % 2],
                    dst_ref=sink.at[1 - o % 2],
                    send_sem=send_sem.at[base + o],
                    recv_sem=recv_sem.at[base + (o ^ 1)],
                    device_id=target,
                    device_id_type=MESH,
                )
            )
        return out

    round1 = copies((snd1t, snd1f), (rcv1t, rcv1f), 0)
    for copy in round1:
        copy.start()

    v = expanded(slots_s, own16)
    q = expanded(codes_s, own16)
    side, pos = v >> 3, v & 7
    their, turned = q >> 1, (q & 1) == 1
    send16, recv16 = send_row(v, own16), recv_row(v)
    point = lane8 & 15
    a_at, b_at = point & 3, point >> 2
    place = jnp.where((sub8 & 1) == 0, a_at, b_at)
    on_edge = (
        ((sub8 == 0) & (b_at == 0))
        | ((sub8 == 1) & (a_at == 3))
        | ((sub8 == 2) & (b_at == 3))
        | ((sub8 == 3) & (a_at == 0))
    )
    there = jnp.where(turned, 3 - place, place)
    cell_a = jnp.where(their == 1, 1, jnp.where(their == 2, 2, 0))
    cell_b = jnp.where(their == 0, 1, jnp.where(their == 3, 2, 3))
    inside = side == 0
    near = [
        jnp.where(inside, 4 * pos + jnp.where(turned, cell_b, cell_a), NOWHERE),
        jnp.where(inside, 4 * pos + jnp.where(turned, cell_a, cell_b), NOWHERE),
    ]
    flip = q & 1
    far = [recv16 + flip, recv16 + 1 - flip]
    send_point = jnp.where(on_edge, 2 * send16 + place, NOWHERE)
    recv_point = jnp.where(on_edge, 2 * recv16 + there, NOWHERE)
    near_point = jnp.where(
        on_edge & inside,
        16 * pos
        + jnp.where((their & 1) == 1, 4 * there, there)
        + jnp.where(their == 1, 3, jnp.where(their == 2, 12, 0)),
        NOWHERE,
    )
    mass = mass_ref[...]
    table = table_ref[...] * mass
    i32 = iota((32, 128), 0)
    i48 = iota((48, 128), 0)
    i128 = iota((128, 128), 0)
    r_on = jnp.zeros((32, 128), F32)
    r_far = jnp.zeros((24, 128), F32)
    sel2 = jnp.zeros((48, 128), F32)
    q_far = jnp.zeros((48, 128), F32)
    q_on = jnp.where(i128 == lane8[0:1], 1.0, 0.0)
    for c in range(4):
        r_on = r_on + jnp.where(i32 == 4 * own16[0:1] + c, table[c : c + 1], 0.0)
    for k in range(4):
        for m in range(2):
            weight = table[4 + 2 * k + m : 5 + 2 * k + m]
            r_on = r_on + jnp.where(i32 == near[m][k : k + 1], weight, 0.0)
            r_far = r_far + jnp.where(i24 == far[m][k : k + 1], weight, 0.0)
        sel2 = sel2 + jnp.where(i48 == send_point[k : k + 1], 1.0, 0.0)
        q_far = q_far + jnp.where(i48 == recv_point[k : k + 1], 1.0, 0.0)
        q_on = q_on + jnp.where(i128 == near_point[k : k + 1], 1.0, 0.0)

    recv4 = recv_row(v4)
    turned4 = (expanded(codes_s, own4) & 1) == 1
    nodes = [-1.0, -1.0 / math.sqrt(5.0), 1.0 / math.sqrt(5.0), 1.0]
    own_add = jnp.zeros((48, 128), F32)
    for k in range(4):
        values = []
        for node in nodes:
            near_edge = [0.5 * linear_weight(m, node) * lagrange(0, -1.0) for m in range(2)]
            values.append(
                jnp.where(
                    cell == CELL_EDGE[k][0],
                    near_edge[0],
                    jnp.where(cell == CELL_EDGE[k][1], near_edge[1], 0.0),
                )
            )
        for t in range(4):
            value = jnp.where(turned4[k : k + 1], values[3 - t], values[t])
            own_add = own_add + jnp.where(i48 == 2 * recv4[k : k + 1] + t, value, 0.0)
    head, rest = halves(own_add)
    group48 = iota((48, 128), 1) >> 5
    own_add = jnp.where(group48 == 1, rest, jnp.where(group48 == 3, 0.0, head)).astype(BF16)

    sel2_16 = sel2.astype(BF16)
    head, rest = halves(r_on)
    r_on3 = jnp.concatenate([head, rest, head, jnp.zeros((32, 128), F32)], axis=0).astype(BF16)
    head, rest = halves(r_far)
    r_far3 = jnp.concatenate([head, rest, head], axis=0).astype(BF16)
    through_on = dot16(sel2_16, r_on3, NT).astype(BF16)
    through = dot16(sel2_16, r_far3, NT)

    def direction(i):
        return jnp.where(i < 8, 0, jnp.where(i < 16, 1, jnp.where(i < 20, 2, 3)))

    there72 = iota((48, 72), 1)
    there72 = jnp.where(there72 < 24, there72, jnp.where(there72 < 48, there72 - 24, there72 - 48))
    same_way = direction(iota((48, 72), 0) >> 1) == direction(there72)
    through = jnp.where(same_way, 0.0, through).astype(BF16)
    masses = jnp.sum(sel2 * mass, axis=1, keepdims=True)
    lane_wide = iota((48, rows), 1)
    base2 = dot16(through_on, pieces_t, NT) + jnp.where(lane_wide == flat, masses, 0.0)
    added = dot16(own_add, pieces_t, NT)
    both = jnp.concatenate([r_on, r_far, jnp.broadcast_to(mass, (8, 128))], axis=0)
    both = dot(both, q_on, NN)
    head, rest = halves(both[0:32])
    near_on = jnp.concatenate([head, rest, head, jnp.zeros((32, 128), F32)], axis=0).astype(BF16)
    head, rest = halves(both[32:56])
    near_far = jnp.concatenate([head, rest, head], axis=0).astype(BF16)
    w_on[...] = dot16(pieces_t, near_on, NN)
    w_on[flat : flat + 1, :] = both[56:57]

    def passive(tile, carry):
        parts = horizontal_parts(tile)
        for r in range(chunks):
            for f in range(3):
                a = st[3 + f, part(r), lanes(tile)].astype(F32)
                bs[f, part(r, 8), :] = horizontal(a, parts)
        for step in range(NSUB):
            for r in range(chunks):
                for f in range(3):
                    a = vertical(3 * step + f, r)
                    if f == 0:
                        a = a + zs[tile, step, part(r), :]
                    if step + 1 < NSUB:
                        bs[3 * (step + 1) + f, part(r, 8), :] = horizontal(a, parts)
                    else:
                        state_out[3 + f, part(r), lanes(tile)] = a.astype(BF16)
        for f in range(3):
            state_out[f, :, lanes(tile)] = st[f, :, lanes(tile)]
        return carry

    lax.fori_loop(0, tiles, passive, 0)

    round2 = copies((snd2t, snd2f), (rcv2t, rcv2f), 4)

    def halo_pieces(halo):
        head, rest = halves(halo)
        return jnp.concatenate([head, head, rest], axis=0).astype(BF16)

    round1[3].wait_recv()
    round1[2].wait_recv()
    round1[1].wait_recv()
    halo_f = jnp.concatenate([rcv1f[0], rcv1f[1]], axis=0)
    halo = jnp.concatenate([rcv1t[0], jnp.zeros((8, rows), F32), halo_f], axis=0)
    message = base2[16:32] + dot16(through[16:32], halo_pieces(halo), NN)
    snd2t[1] = message
    round2[1].start()
    round1[0].wait_recv()
    halo = jnp.concatenate([rcv1t[0], rcv1t[1], halo_f], axis=0)
    pieces = halo_pieces(halo)
    message = base2 + dot16(through, pieces, NN)
    snd2f[0] = message[32:40]
    snd2f[1] = message[40:48]
    snd2t[0] = message[0:16]
    round2[2].start()
    round2[3].start()
    round2[0].start()
    near_sum = w_on[...] + dot16(pieces, near_far, TN)
    pick = jnp.concatenate([q_far, q_far], axis=0).astype(BF16)
    for copy in round2:
        copy.wait_recv()
    halo2 = jnp.concatenate([rcv2t[0], rcv2t[1], rcv2f[0], rcv2f[1]], axis=0)
    halo2 = halo2 + halo2[:, flat : flat + 1] * added
    total = near_sum + dot16(jnp.concatenate(halves(halo2), axis=0).astype(BF16), pick, TN)
    inverse = 1.0 / total[flat : flat + 1, :]
    for f in range(fields):
        gll_out[f] = total[f * levels : (f + 1) * levels, :] * inverse
    for copy in round1 + round2:
        copy.wait_send()


def local(
    nf,
    nt,
    crm_state,
    active_levels,
    mix_x,
    drift_speed,
    cond_rate,
    mix_z,
    point_mass,
    neighbor_slots,
    edge_codes,
):
    fields, levels, width = crm_state.shape
    flat = fields * levels
    points = point_mass.shape[0]
    wide = 128 * (flat // 128 + 1)
    tiles = width // 128
    matrix = remap_matrix()
    table = np.zeros((16, points), np.float32)
    table[:12] = np.tile(matrix.T, (1, points // 16))
    vmem = pl.BlockSpec(memory_space=pltpu.VMEM)
    hbm = pl.BlockSpec(memory_space=pltpu.HBM)
    state, gll = pl.pallas_call(
        functools.partial(kernel, nf, nt),
        out_shape=(
            jax.ShapeDtypeStruct(crm_state.shape, BF16),
            jax.ShapeDtypeStruct((fields, levels, points), F32),
        ),
        in_specs=[hbm] * 10,
        out_specs=(vmem, vmem),
        scratch_shapes=[
            pltpu.SMEM(neighbor_slots.shape, jnp.int32),
            pltpu.SMEM(edge_codes.shape, jnp.int32),
            pltpu.SMEM(active_levels.shape, jnp.int32),
            pltpu.SMEM(mix_x.shape, F32),
            pltpu.SMEM(drift_speed.shape, F32),
            pltpu.SMEM(cond_rate.shape, F32),
            pltpu.SMEM(mix_z.shape, F32),
            pltpu.VMEM((1, points), F32),
            pltpu.VMEM(table.shape, F32),
            pltpu.VMEM((fields, levels, width), BF16),
            pltpu.VMEM((12, levels + 16, 128), F32),
            pltpu.VMEM((12, levels + 16, 128), F32),
            pltpu.VMEM((3, levels + 16, 128), F32),
            pltpu.VMEM((width, 128), F32),
            pltpu.VMEM((tiles, 2 * levels, 128), F32),
            pltpu.VMEM((tiles, NSUB, levels, 128), F32),
            pltpu.VMEM((fields, levels + 16, 128), F32),
            pltpu.VMEM((2, levels, 128), F32),
            pltpu.VMEM((wide, 128), F32),
            pltpu.VMEM((wide, 128), F32),
            pltpu.VMEM((2, 8, wide), F32),
            pltpu.VMEM((2, 4, wide), F32),
            pltpu.VMEM((2, 16, wide), F32),
            pltpu.VMEM((2, 8, wide), F32),
            pltpu.VMEM((2, 8, wide), F32),
            pltpu.VMEM((2, 4, wide), F32),
            pltpu.VMEM((2, 16, wide), F32),
            pltpu.VMEM((2, 8, wide), F32),
            pltpu.SemaphoreType.DMA((tiles // 2,)),
            pltpu.SemaphoreType.DMA((9,)),
            pltpu.SemaphoreType.DMA((8,)),
            pltpu.SemaphoreType.DMA((8,)),
        ],
        compiler_params=pltpu.CompilerParams(collective_id=0, has_side_effects=True, vmem_limit_bytes=40 << 20),
    )(
        *(
            pltpu.with_memory_space_constraint(x, pltpu.HBM)
            for x in (
                neighbor_slots,
                edge_codes,
                active_levels,
                mix_x,
                drift_speed,
                cond_rate,
                mix_z,
                point_mass.reshape(1, points),
                jnp.asarray(table),
                crm_state,
            )
        )
    )
    return pl.pallas_call(
        write_out,
        out_shape=(
            jax.ShapeDtypeStruct(state.shape, BF16),
            jax.ShapeDtypeStruct(gll.shape, F32),
        ),
        in_specs=[vmem, vmem],
        out_specs=(hbm, hbm),
        scratch_shapes=[pltpu.SemaphoreType.DMA((2,))],
        compiler_params=pltpu.CompilerParams(vmem_limit_bytes=1 << 20),
    )(state, gll)


def write_out(state, gll, state_out, gll_out, sem):
    first = pltpu.make_async_copy(state, state_out, sem.at[0])
    second = pltpu.make_async_copy(gll, gll_out, sem.at[1])
    first.start()
    second.start()
    first.wait()
    second.wait()


def solution(mesh):
    in_specs = (
        P(None, None, ("face", "tile")),
        P(("face", "tile")),
        P(("face", "tile")),
        P(("face", "tile")),
        P(("face", "tile")),
        P(),
        P(("face", "tile")),
        P(None, ("face", "tile")),
        P(None, ("face", "tile")),
    )
    out_specs = (P(None, None, ("face", "tile")), P(None, None, ("face", "tile")))
    body = functools.partial(local, mesh.shape["face"], mesh.shape["tile"])
    return jax.shard_map(body, mesh=mesh, in_specs=in_specs, out_specs=out_specs, check_vma=False)
```

```python
import functools
import math

import jax
import jax.numpy as jnp
import numpy as np
from jax import lax
from jax.experimental import pallas as pl
from jax.experimental.pallas import tpu as pltpu
from jax.sharding import PartitionSpec as P

NSUB = 2
PER_TIME = 10.0
CELL_EDGE = [[0, 1], [1, 3], [2, 3], [0, 2]]
MESH = pl.DeviceIdType.MESH
F32 = jnp.float32
BF16 = jnp.bfloat16
NOWHERE = -100000
LEAST_ACTIVE = 18
EXP_RATE = 0.3 / math.log(2.0)
NN = (((1,), (0,)), ((), ()))
NT = (((1,), (1,)), ((), ()))
TN = (((0,), (0,)), ((), ()))


def lagrange(q, z):
    centres = [-1.5, -0.5, 0.5, 1.5]
    product = 1.0
    for r in range(4):
        if r != q:
            product = product * (z - centres[r]) / (centres[q] - centres[r])
    return product


def linear_weight(j, z):
    return 0.5 - z if j == 0 else 0.5 + z


def remap_matrix():
    gll_nodes = [-1.0, -1.0 / math.sqrt(5.0), 1.0 / math.sqrt(5.0), 1.0]
    matrix = np.zeros((16, 12))
    for b in range(4):
        for a in range(4):
            p = 4 * b + a
            x = gll_nodes[a]
            y = gll_nodes[b]
            for j in range(2):
                for i in range(2):
                    matrix[p, 2 * j + i] += 0.5 * linear_weight(j, y) * lagrange(
                        1 + i, x
                    ) + 0.5 * linear_weight(i, x) * lagrange(1 + j, y)
            for m in range(2):
                matrix[p, 4 + 6 + m] += 0.5 * linear_weight(m, y) * lagrange(0, x)
                matrix[p, 4 + 2 + m] += 0.5 * linear_weight(m, y) * lagrange(3, x)
                matrix[p, 4 + 0 + m] += 0.5 * linear_weight(m, x) * lagrange(0, y)
                matrix[p, 4 + 4 + m] += 0.5 * linear_weight(m, x) * lagrange(3, y)
    return matrix


def iota(shape, dim):
    return lax.broadcasted_iota(jnp.int32, shape, dim)


def dot(a, b, dims):
    return lax.dot_general(
        a, b, dims, precision=lax.Precision.HIGHEST, preferred_element_type=F32
    )


def dot16(a, b, dims):
    return lax.dot_general(a, b, dims, preferred_element_type=F32)


def halves(x):
    head = x.astype(BF16).astype(F32)
    return head, x - head


def kernel(
    nf,
    nt,
    slots_hbm,
    codes_hbm,
    active_hbm,
    mix_hbm,
    drift_hbm,
    cond_hbm,
    mixz_hbm,
    mass_hbm,
    table_hbm,
    crm_hbm,
    state_out,
    gll_out,
    slots_s,
    codes_s,
    active_s,
    mix_s,
    drift_s,
    cond_s,
    mixz_s,
    mass_ref,
    table_ref,
    st,
    bs,
    fs,
    cf,
    ones,
    xs,
    zs,
    acc0,
    acc1,
    tend,
    w_on,
    snd1t,
    snd1f,
    snd2t,
    snd2f,
    rcv1t,
    rcv1f,
    rcv2t,
    rcv2f,
    load_sem,
    small_sem,
    send_sem,
    recv_sem,
):
    fields, levels, width = st.shape
    flat = fields * levels
    tiles = width // 128
    rows = tend.shape[0]
    fi = lax.axis_index("face")
    ti = lax.axis_index("tile")
    targets = [
        (fi, lax.rem(ti + nt - 1, nt)),
        (fi, lax.rem(ti + 1, nt)),
        (lax.rem(fi + nf - 1, nf), ti),
        (lax.rem(fi + 1, nf), ti),
    ]
    loads = []
    for p in range(tiles // 2):
        two = slice(256 * p, 256 * (p + 1))
        loads.append(
            pltpu.make_async_copy(crm_hbm.at[:, :, two], st.at[:, :, two], load_sem.at[p])
        )
    loads[0].start()
    smalls = []
    for n, (source, sink) in enumerate(
        (
            (mixz_hbm, mixz_s),
            (mix_hbm, mix_s),
            (drift_hbm, drift_s),
            (cond_hbm, cond_s),
            (active_hbm, active_s),
            (slots_hbm, slots_s),
            (codes_hbm, codes_s),
            (mass_hbm, mass_ref),
            (table_hbm, table_ref),
        )
    ):
        smalls.append(pltpu.make_async_copy(source, sink, small_sem.at[n]))
        smalls[-1].start()
    for copy in loads[1:]:
        copy.start()
    barrier = pltpu.get_barrier_semaphore()
    for target in targets:
        pl.semaphore_signal(barrier, inc=1, device_id=target, device_id_type=MESH)

    lane8 = iota((8, 128), 1)
    sub8 = iota((8, 128), 0)

    own16 = lane8 >> 4
    own4 = (lane8 & 31) >> 2

    def expanded(source, own):
        key = sub8 * 32 + own
        out = jnp.full((8, 128), -1, jnp.int32)
        for k in range(4):
            for e in range(8):
                out = jnp.where(key == k * 32 + e, source[k, e], out)
        return out

    def base_of(side):
        return jnp.where(
            side == 1,
            0,
            jnp.where(side == 2, 8, jnp.where(side == 3, 16, jnp.where(side == 4, 20, NOWHERE))),
        )

    def send_row(v, own):
        side = v >> 3
        rank = jnp.zeros((8, 128), jnp.int32)
        for k in range(4):
            for e in range(8):
                rank = rank + jnp.where((side == (slots_s[k, e] >> 3)) & (own > e), 2, 0)
        return base_of(side) + rank

    def recv_row(v):
        side = v >> 3
        rank = jnp.zeros((8, 128), jnp.int32)
        for k in range(4):
            for e in range(8):
                other = slots_s[k, e]
                rank = rank + jnp.where((side == (other >> 3)) & (v > other), 2, 0)
        return base_of(side) + rank

    lane_r = iota((256, 128), 0) >> 5
    lane_n = iota((256, 128), 1) & 31
    for p in range(width // 256):
        ones[256 * p : 256 * (p + 1), :] = jnp.where(lane_n == lane_r + 8 * p, 1.0, 0.0)
    acc0[...] = jnp.zeros_like(acc0)
    acc1[...] = jnp.zeros_like(acc1)
    tend[flat:rows, :] = jnp.zeros((rows - flat, 128), F32)
    blank = jnp.zeros((8, 128), F32)
    for n in range(bs.shape[0]):
        bs[n, 0:8, :] = blank
        bs[n, levels + 8 : levels + 16, :] = blank
        fs[n, 0:8, :] = blank
    for n in range(cf.shape[0]):
        cf[n, 0:8, :] = blank
        cf[n, levels + 8 : levels + 16, :] = blank

    for copy in smalls:
        copy.wait()

    chunks = levels // 8
    for r in range(chunks):
        upper, lower = blank, blank
        for s in range(8):
            l = 8 * r + s
            if l < levels - 1:
                upper = jnp.where(sub8 == s, mixz_s[l], upper)
            if l > 0:
                lower = jnp.where(sub8 == s, mixz_s[l - 1], lower)
        cf[0, 8 * r + 8 : 8 * r + 16, :] = upper
        cf[1, 8 * r + 8 : 8 * r + 16, :] = lower
        cf[2, 8 * r + 8 : 8 * r + 16, :] = 1.0 - upper - lower

    def part(r, shift=0):
        return slice(8 * r + shift, 8 * r + 8 + shift)

    def vertical(n, r):
        b = bs[n, part(r, 8), :]
        flux = cf[0, part(r, 8), :] * (bs[n, part(r, 9), :] - b)
        fs[n, part(r, 8), :] = flux
        return b + flux - fs[n, part(r, 7), :]

    east_at = (lane8 & 96) | ((lane8 + 1) & 31)
    west_at = (lane8 & 96) | ((lane8 + 31) & 31)
    group = lane8 >> 5

    def per_column(source, tile):
        out = jnp.full((8, 128), source[4 * tile])
        for g in range(1, 4):
            out = jnp.where(group == g, source[4 * tile + g], out)
        return out

    def horizontal_parts(tile):
        mix = per_column(mix_s, tile)
        half = 0.5 * per_column(drift_s, tile)
        return 1.0 - 2.0 * mix, mix - half, mix + half

    def horizontal(a, parts):
        mid, east, west = parts
        return (
            a * mid
            + east * jnp.take_along_axis(a, east_at, axis=1)
            + west * jnp.take_along_axis(a, west_at, axis=1)
        )

    def lanes(tile):
        return pl.ds(pl.multiple_of(tile * 128, 128), 128)

    def gather_sums(slot, tile):
        head, rest = halves(xs[slot])
        pick = ones[128 * tile : 128 * (tile + 1), :]
        sums = dot16(
            jnp.concatenate([head, rest], axis=1), jnp.concatenate([pick, pick], axis=0), NN
        )
        for n in range(2):
            acc1[n] += sums[n * levels : (n + 1) * levels]

    def active_tile(tile, slot, lot, chunk):
        parts = horizontal_parts(tile)
        limit = per_column(active_s, tile)
        rate = per_column(cond_s, tile)
        at_lanes = slice(128 * tile, 128 * (tile + 1))
        for r in range(chunks):
            for f in range(3):
                bs[lot + f, part(r, 8), :] = horizontal(chunk[f][r], parts)
        for step in range(NSUB):
            for r in range(chunks):
                t, qv, ql = (vertical(lot + 3 * step + f, r) for f in range(3))
                always = 8 * r + 8 <= LEAST_ACTIVE
                alive = sub8 + 8 * r < limit
                sat = jnp.exp2(EXP_RATE * t - 1.0)
                cond = jnp.maximum(rate * (qv - sat), -ql)
                if not always:
                    cond = jnp.where(alive, cond, 0.0)
                qv = qv - cond
                ql = ql + cond
                t = t + 0.5 * cond
                freeze = 0.15 * ql * (1.0 - jnp.tanh(t))
                if not always:
                    freeze = jnp.where(alive, freeze, 0.0)
                ql = ql - freeze
                t = t + 0.1 * freeze
                zs[tile, step, part(r), :] = freeze
                if step + 1 < NSUB:
                    for f, a in enumerate((t, qv, ql)):
                        bs[lot + 3 * (step + 1) + f, part(r, 8), :] = horizontal(a, parts)
                else:
                    xs[slot, 8 * r : 8 * r + 8, :] = qv
                    xs[slot, levels + 8 * r : levels + 8 * r + 8, :] = ql
                    for f, a in enumerate((t, qv, ql)):
                        st[f, part(r), at_lanes] = a.astype(BF16)

    for p in range(tiles // 2):
        if p < 2:
            for copy in loads[p : (1, tiles // 2)[p]]:
                copy.wait()
        if p == 0:
            v4 = expanded(slots_s, own4)
            row4 = jnp.where((lane8 & 32) == 0, send_row(v4, own4), NOWHERE)
            cell = lane8[0:1] & 3
            i24 = iota((24, 128), 0)
            sel1 = jnp.zeros((24, 128), F32)
            for k in range(4):
                first = row4[k : k + 1]
                goal = jnp.where(
                    cell == CELL_EDGE[k][0],
                    first,
                    jnp.where(cell == CELL_EDGE[k][1], first + 1, NOWHERE),
                )
                sel1 = sel1 + jnp.where(i24 == goal, 1.0, 0.0)

        chunk = [
            [
                [
                    st[f, part(r), 128 * tile : 128 * (tile + 1)].astype(F32)
                    for r in range(chunks)
                ]
                for f in range(fields)
            ]
            for tile in (2 * p, 2 * p + 1)
        ]
        start = jnp.concatenate(
            [
                jnp.concatenate([chunk[0][f][r], chunk[1][f][r]], axis=1)
                for f in range(fields)
                for r in range(chunks)
            ],
            axis=0,
        )
        sums = dot16(start, ones[256 * p : 256 * (p + 1), :], NN)
        for f in range(fields):
            acc0[f, 8 : levels + 8, :] += sums[f * levels : (f + 1) * levels]
        for tile in (2 * p, 2 * p + 1):
            if tile >= 2:
                gather_sums(tile - 2, tile - 2)
            active_tile(tile, tile, 6 * (tile % 2), chunk[tile % 2])
    gather_sums(tiles - 2, tiles - 2)
    gather_sums(tiles - 1, tiles - 1)

    scale = PER_TIME / 32.0
    for r in range(chunks):
        upper, lower, middle = (cf[n, part(r, 8), :] for n in range(3))
        two_up = scale * upper * cf[0, part(r, 9), :]
        one_up = scale * upper * (middle + cf[2, part(r, 9), :])
        one_down = scale * lower * (middle + cf[2, part(r, 7), :])
        two_down = scale * lower * cf[1, part(r, 7), :]
        same = scale * (upper * upper + lower * lower + middle * middle - 1.0)
        mixed = []
        for f in range(fields):
            mixed.append(
                same * acc0[f, part(r, 8), :]
                + (one_up * acc0[f, part(r, 9), :] + one_down * acc0[f, part(r, 7), :])
                + (two_up * acc0[f, part(r, 10), :] + two_down * acc0[f, part(r, 6), :])
            )
        vapour = scale * (acc1[0, part(r), :] - acc0[1, part(r, 8), :])
        liquid = scale * (acc1[1, part(r), :] - acc0[2, part(r, 8), :])
        cond_sum = mixed[1] - vapour
        freeze_sum = mixed[2] + cond_sum - liquid
        mixed[0] = mixed[0] + 0.5 * cond_sum + 0.1 * freeze_sum
        mixed[1] = vapour
        mixed[2] = liquid
        mixed[3] = mixed[3] + freeze_sum
        for f in range(fields):
            at = f * levels + 8 * r
            tend[at : at + 8, :] = mixed[f]

    head, rest = halves(tend[...])
    wide_group = iota((rows, 128), 1) >> 5
    pieces_t = jnp.where(wide_group < 2, head, rest).astype(BF16)
    message = dot16(sel1.astype(BF16), pieces_t, NT)
    snd1t[0] = message[0:8]
    snd1t[1] = message[8:16]
    snd1f[0] = message[16:20]
    snd1f[1] = message[20:24]

    pl.semaphore_wait(barrier, 4)

    def copies(sends, recvs, base):
        out = []
        for o, target in enumerate(targets):
            source, sink = (sends[0], recvs[0]) if o < 2 else (sends[1], recvs[1])
            out.append(
                pltpu.make_async_remote_copy(
                    src_ref=source.at[o % 2],
                    dst_ref=sink.at[1 - o % 2],
                    send_sem=send_sem.at[base + o],
                    recv_sem=recv_sem.at[base + (o ^ 1)],
                    device_id=target,
                    device_id_type=MESH,
                )
            )
        return out

    round1 = copies((snd1t, snd1f), (rcv1t, rcv1f), 0)
    for copy in round1:
        copy.start()

    v = expanded(slots_s, own16)
    q = expanded(codes_s, own16)
    side, pos = v >> 3, v & 7
    their, turned = q >> 1, (q & 1) == 1
    send16, recv16 = send_row(v, own16), recv_row(v)
    point = lane8 & 15
    a_at, b_at = point & 3, point >> 2
    place = jnp.where((sub8 & 1) == 0, a_at, b_at)
    on_edge = (
        ((sub8 == 0) & (b_at == 0))
        | ((sub8 == 1) & (a_at == 3))
        | ((sub8 == 2) & (b_at == 3))
        | ((sub8 == 3) & (a_at == 0))
    )
    there = jnp.where(turned, 3 - place, place)
    cell_a = jnp.where(their == 1, 1, jnp.where(their == 2, 2, 0))
    cell_b = jnp.where(their == 0, 1, jnp.where(their == 3, 2, 3))
    inside = side == 0
    near = [
        jnp.where(inside, 4 * pos + jnp.where(turned, cell_b, cell_a), NOWHERE),
        jnp.where(inside, 4 * pos + jnp.where(turned, cell_a, cell_b), NOWHERE),
    ]
    flip = q & 1
    far = [recv16 + flip, recv16 + 1 - flip]
    send_point = jnp.where(on_edge, 2 * send16 + place, NOWHERE)
    recv_point = jnp.where(on_edge, 2 * recv16 + there, NOWHERE)
    near_point = jnp.where(
        on_edge & inside,
        16 * pos
        + jnp.where((their & 1) == 1, 4 * there, there)
        + jnp.where(their == 1, 3, jnp.where(their == 2, 12, 0)),
        NOWHERE,
    )
    mass = mass_ref[...]
    table = table_ref[...] * mass
    i32 = iota((32, 128), 0)
    i48 = iota((48, 128), 0)
    i128 = iota((128, 128), 0)
    r_on = jnp.zeros((32, 128), F32)
    r_far = jnp.zeros((24, 128), F32)
    sel2 = jnp.zeros((48, 128), F32)
    q_far = jnp.zeros((48, 128), F32)
    q_on = jnp.where(i128 == lane8[0:1], 1.0, 0.0)
    for c in range(4):
        r_on = r_on + jnp.where(i32 == 4 * own16[0:1] + c, table[c : c + 1], 0.0)
    for k in range(4):
        for m in range(2):
            weight = table[4 + 2 * k + m : 5 + 2 * k + m]
            r_on = r_on + jnp.where(i32 == near[m][k : k + 1], weight, 0.0)
            r_far = r_far + jnp.where(i24 == far[m][k : k + 1], weight, 0.0)
        sel2 = sel2 + jnp.where(i48 == send_point[k : k + 1], 1.0, 0.0)
        q_far = q_far + jnp.where(i48 == recv_point[k : k + 1], 1.0, 0.0)
        q_on = q_on + jnp.where(i128 == near_point[k : k + 1], 1.0, 0.0)

    recv4 = recv_row(v4)
    turned4 = (expanded(codes_s, own4) & 1) == 1
    nodes = [-1.0, -1.0 / math.sqrt(5.0), 1.0 / math.sqrt(5.0), 1.0]
    own_add = jnp.zeros((48, 128), F32)
    for k in range(4):
        values = []
        for node in nodes:
            near_edge = [0.5 * linear_weight(m, node) * lagrange(0, -1.0) for m in range(2)]
            values.append(
                jnp.where(
                    cell == CELL_EDGE[k][0],
                    near_edge[0],
                    jnp.where(cell == CELL_EDGE[k][1], near_edge[1], 0.0),
                )
            )
        for t in range(4):
            value = jnp.where(turned4[k : k + 1], values[3 - t], values[t])
            own_add = own_add + jnp.where(i48 == 2 * recv4[k : k + 1] + t, value, 0.0)
    head, rest = halves(own_add)
    group48 = iota((48, 128), 1) >> 5
    own_add = jnp.where(group48 == 1, rest, jnp.where(group48 == 3, 0.0, head)).astype(BF16)

    sel2_16 = sel2.astype(BF16)
    head, rest = halves(r_on)
    r_on3 = jnp.concatenate([head, rest, head, jnp.zeros((32, 128), F32)], axis=0).astype(BF16)
    head, rest = halves(r_far)
    r_far3 = jnp.concatenate([head, rest, head], axis=0).astype(BF16)
    through_on = dot16(sel2_16, r_on3, NT).astype(BF16)
    through = dot16(sel2_16, r_far3, NT)

    def direction(i):
        return jnp.where(i < 8, 0, jnp.where(i < 16, 1, jnp.where(i < 20, 2, 3)))

    there72 = iota((48, 72), 1)
    there72 = jnp.where(there72 < 24, there72, jnp.where(there72 < 48, there72 - 24, there72 - 48))
    same_way = direction(iota((48, 72), 0) >> 1) == direction(there72)
    through = jnp.where(same_way, 0.0, through).astype(BF16)
    masses = jnp.sum(sel2 * mass, axis=1, keepdims=True)
    lane_wide = iota((48, rows), 1)
    base2 = dot16(through_on, pieces_t, NT) + jnp.where(lane_wide == flat, masses, 0.0)
    added = dot16(own_add, pieces_t, NT)
    both = jnp.concatenate([r_on, r_far, jnp.broadcast_to(mass, (8, 128))], axis=0)
    both = dot(both, q_on, NN)
    head, rest = halves(both[0:32])
    near_on = jnp.concatenate([head, rest, head, jnp.zeros((32, 128), F32)], axis=0).astype(BF16)
    head, rest = halves(both[32:56])
    near_far = jnp.concatenate([head, rest, head], axis=0).astype(BF16)
    w_on[...] = dot16(pieces_t, near_on, NN)
    w_on[flat : flat + 1, :] = both[56:57]

    def passive(tile, carry):
        parts = horizontal_parts(tile)
        for r in range(chunks):
            for f in range(3):
                a = st[3 + f, part(r), lanes(tile)].astype(F32)
                bs[f, part(r, 8), :] = horizontal(a, parts)
        for step in range(NSUB):
            for r in range(chunks):
                for f in range(3):
                    a = vertical(3 * step + f, r)
                    if f == 0:
                        a = a + zs[tile, step, part(r), :]
                    if step + 1 < NSUB:
                        bs[3 * (step + 1) + f, part(r, 8), :] = horizontal(a, parts)
                    else:
                        state_out[3 + f, part(r), lanes(tile)] = a.astype(BF16)
        for f in range(3):
            state_out[f, :, lanes(tile)] = st[f, :, lanes(tile)]
        return carry

    lax.fori_loop(0, tiles, passive, 0)

    round2 = copies((snd2t, snd2f), (rcv2t, rcv2f), 4)

    def halo_pieces(halo):
        head, rest = halves(halo)
        return jnp.concatenate([head, head, rest], axis=0).astype(BF16)

    low_half = lane8 < 64
    full = rows // 128 - 1

    def pack(sink, message):
        for j in range(full):
            sink[16 * j : 16 * j + 16, :] = message[:, 128 * j : 128 * (j + 1)]
        end = message[:, 128 * full :]
        sink[16 * full : 16 * full + 8, :] = jnp.where(
            low_half, end[0:8], pltpu.roll(end[8:16], 64, 1)
        )

    def unpack(source):
        end = source[16 * full : 16 * full + 8, :]
        end = jnp.concatenate([end, pltpu.roll(end, 64, 1)], axis=0)
        return jnp.concatenate(
            [source[16 * j : 16 * j + 16, :] for j in range(full)] + [end], axis=1
        )

    round1[3].wait_recv()
    round1[2].wait_recv()
    round1[1].wait_recv()
    halo_f = jnp.concatenate([rcv1f[0], rcv1f[1]], axis=0)
    halo = jnp.concatenate([rcv1t[0], jnp.zeros((8, rows), F32), halo_f], axis=0)
    message = base2[16:32] + dot16(through[16:32], halo_pieces(halo), NN)
    pack(snd2t.at[1], message)
    round2[1].start()
    round1[0].wait_recv()
    halo = jnp.concatenate([rcv1t[0], rcv1t[1], halo_f], axis=0)
    pieces = halo_pieces(halo)
    message = base2 + dot16(through, pieces, NN)
    snd2f[0] = message[32:40]
    snd2f[1] = message[40:48]
    pack(snd2t.at[0], message[0:16])
    round2[2].start()
    round2[3].start()
    round2[0].start()
    near_sum = w_on[...] + dot16(pieces, near_far, TN)
    pick = jnp.concatenate([q_far, q_far], axis=0).astype(BF16)
    for copy in round2:
        copy.wait_recv()
    halo2 = jnp.concatenate([unpack(rcv2t.at[0]), unpack(rcv2t.at[1]), rcv2f[0], rcv2f[1]], axis=0)
    halo2 = halo2 + halo2[:, flat : flat + 1] * added
    total = near_sum + dot16(jnp.concatenate(halves(halo2), axis=0).astype(BF16), pick, TN)
    inverse = 1.0 / total[flat : flat + 1, :]
    for f in range(fields):
        gll_out[f] = total[f * levels : (f + 1) * levels, :] * inverse
    for copy in round1 + round2:
        copy.wait_send()


def local(
    nf,
    nt,
    crm_state,
    active_levels,
    mix_x,
    drift_speed,
    cond_rate,
    mix_z,
    point_mass,
    neighbor_slots,
    edge_codes,
):
    fields, levels, width = crm_state.shape
    flat = fields * levels
    points = point_mass.shape[0]
    wide = 128 * (flat // 128 + 1)
    assert flat % 128 < 64
    tiles = width // 128
    matrix = remap_matrix()
    table = np.zeros((16, points), np.float32)
    table[:12] = np.tile(matrix.T, (1, points // 16))
    vmem = pl.BlockSpec(memory_space=pltpu.VMEM)
    hbm = pl.BlockSpec(memory_space=pltpu.HBM)
    state, gll = pl.pallas_call(
        functools.partial(kernel, nf, nt),
        out_shape=(
            jax.ShapeDtypeStruct(crm_state.shape, BF16),
            jax.ShapeDtypeStruct((fields, levels, points), F32),
        ),
        in_specs=[hbm] * 10,
        out_specs=(vmem, vmem),
        scratch_shapes=[
            pltpu.SMEM(neighbor_slots.shape, jnp.int32),
            pltpu.SMEM(edge_codes.shape, jnp.int32),
            pltpu.SMEM(active_levels.shape, jnp.int32),
            pltpu.SMEM(mix_x.shape, F32),
            pltpu.SMEM(drift_speed.shape, F32),
            pltpu.SMEM(cond_rate.shape, F32),
            pltpu.SMEM(mix_z.shape, F32),
            pltpu.VMEM((1, points), F32),
            pltpu.VMEM(table.shape, F32),
            pltpu.VMEM((fields, levels, width), BF16),
            pltpu.VMEM((12, levels + 16, 128), F32),
            pltpu.VMEM((12, levels + 16, 128), F32),
            pltpu.VMEM((3, levels + 16, 128), F32),
            pltpu.VMEM((width, 128), F32),
            pltpu.VMEM((tiles, 2 * levels, 128), F32),
            pltpu.VMEM((tiles, NSUB, levels, 128), F32),
            pltpu.VMEM((fields, levels + 16, 128), F32),
            pltpu.VMEM((2, levels, 128), F32),
            pltpu.VMEM((wide, 128), F32),
            pltpu.VMEM((wide, 128), F32),
            pltpu.VMEM((2, 8, wide), F32),
            pltpu.VMEM((2, 4, wide), F32),
            pltpu.VMEM((2, wide // 8 - 8, 128), F32),
            pltpu.VMEM((2, 8, wide), F32),
            pltpu.VMEM((2, 8, wide), F32),
            pltpu.VMEM((2, 4, wide), F32),
            pltpu.VMEM((2, wide // 8 - 8, 128), F32),
            pltpu.VMEM((2, 8, wide), F32),
            pltpu.SemaphoreType.DMA((tiles // 2,)),
            pltpu.SemaphoreType.DMA((9,)),
            pltpu.SemaphoreType.DMA((8,)),
            pltpu.SemaphoreType.DMA((8,)),
        ],
        compiler_params=pltpu.CompilerParams(collective_id=0, has_side_effects=True, vmem_limit_bytes=40 << 20),
    )(
        *(
            pltpu.with_memory_space_constraint(x, pltpu.HBM)
            for x in (
                neighbor_slots,
                edge_codes,
                active_levels,
                mix_x,
                drift_speed,
                cond_rate,
                mix_z,
                point_mass.reshape(1, points),
                jnp.asarray(table),
                crm_state,
            )
        )
    )
    return pl.pallas_call(
        write_out,
        out_shape=(
            jax.ShapeDtypeStruct(state.shape, BF16),
            jax.ShapeDtypeStruct(gll.shape, F32),
        ),
        in_specs=[vmem, vmem],
        out_specs=(hbm, hbm),
        scratch_shapes=[pltpu.SemaphoreType.DMA((2,))],
        compiler_params=pltpu.CompilerParams(vmem_limit_bytes=1 << 20),
    )(state, gll)


def write_out(state, gll, state_out, gll_out, sem):
    first = pltpu.make_async_copy(state, state_out, sem.at[0])
    second = pltpu.make_async_copy(gll, gll_out, sem.at[1])
    first.start()
    second.start()
    first.wait()
    second.wait()


def solution(mesh):
    in_specs = (
        P(None, None, ("face", "tile")),
        P(("face", "tile")),
        P(("face", "tile")),
        P(("face", "tile")),
        P(("face", "tile")),
        P(),
        P(("face", "tile")),
        P(None, ("face", "tile")),
        P(None, ("face", "tile")),
    )
    out_specs = (P(None, None, ("face", "tile")), P(None, None, ("face", "tile")))
    body = functools.partial(local, mesh.shape["face"], mesh.shape["tile"])
    return jax.shard_map(body, mesh=mesh, in_specs=in_specs, out_specs=out_specs, check_vma=False)
```
